128 devices in a mesh: dy: 4 (over x), dx: 32 (over z, y, core).
Axes of the slice: x: 4, y: 4, z: 4, core: 2. Of those that a mesh axis runs over, the one named last changes fastest.
Arguments:
- tokens: bfloat16 [32768, 1024], P(('dy', 'dx'))
- targets: bfloat16 [32768, 1024], P(('dy', 'dx'))
- w_in: bfloat16 [4, 1024, 4096], replicated
- w_out: bfloat16 [4, 4096, 1024], replicated
Outputs:
- output 1: float32 [4, 1024, 4096], replicated
- output 2: float32 [4, 4096, 1024], replicated
All inputs are finite; a program needn't handle non-finite values.
Results may differ from the reference program's by a relative error of at most 0.00957852.
Values are sent between devices in bfloat16 or wider.
A program may use at most 1 GiB of HBM per device.

```python
import jax
import jax.numpy as jnp
from jax import lax

D = 1024
FF = 4096
TOK = 256
LAYERS = 4
SHARDS = 128


def setup_inputs(seed: int = 0) -> dict:
    total_tok = SHARDS * TOK
    rng_keys = jax.random.split(jax.random.key(seed), 4)
    targ_scale = 0.5 * total_tok ** 0.5
    tokens = jax.random.normal(rng_keys[0], (total_tok, D), jnp.float32)
    targets = jax.random.normal(rng_keys[1], (total_tok, D), jnp.float32) * targ_scale
    w_in = jax.random.normal(rng_keys[2], (LAYERS, D, FF), jnp.float32) * D ** -0.5
    w_out = jax.random.normal(rng_keys[3], (LAYERS, FF, D), jnp.float32) * FF ** -0.5
    return {'tokens': tokens.astype(jnp.bfloat16), 'targets': targets.astype(jnp.bfloat16), 'w_in': w_in.astype(jnp.bfloat16), 'w_out': w_out.astype(jnp.bfloat16)}


def shard_grads(tok_shard, tgt_shard, w_in, w_out):
    inv_total = 1.0 / (SHARDS * TOK)

    def forward_layer(hidden, layer_weights):
        w_first, w_second = layer_weights
        pre_act = jnp.dot(hidden, w_first, preferred_element_type=jnp.float32).astype(jnp.bfloat16)
        post_act = jax.nn.gelu(pre_act.astype(jnp.float32)).astype(jnp.bfloat16)
        branch = jnp.dot(post_act, w_second, preferred_element_type=jnp.float32)
        hidden_next = (hidden.astype(jnp.float32) + branch).astype(jnp.bfloat16)
        return hidden_next, (hidden, pre_act, post_act)

    final, saved = lax.scan(forward_layer, tok_shard, (w_in, w_out))
    grad_top = ((final.astype(jnp.float32) - tgt_shard.astype(jnp.float32)) * inv_total).astype(jnp.bfloat16)

    def backward_layer(grad_hid, layer_data):
        hidden, pre_act, post_act, w_first, w_second = layer_data
        grad_w_out = jnp.dot(post_act.T, grad_hid, preferred_element_type=jnp.float32)
        grad_post = jnp.dot(grad_hid, w_second.T, preferred_element_type=jnp.float32)
        gelu_vjp = jax.vjp(jax.nn.gelu, pre_act.astype(jnp.float32))[1]
        grad_pre = gelu_vjp(grad_post)[0].astype(jnp.bfloat16)
        grad_w_in = jnp.dot(hidden.T, grad_pre, preferred_element_type=jnp.float32)
        through_w = jnp.dot(grad_pre, w_first.T, preferred_element_type=jnp.float32)
        grad_below = (grad_hid.astype(jnp.float32) + through_w).astype(jnp.bfloat16)
        return grad_below, (grad_w_in, grad_w_out)

    hiddens, pre_acts, post_acts = saved
    layer_grads = lax.scan(backward_layer, grad_top, (hiddens, pre_acts, post_acts, w_in, w_out), reverse=True)[1]
    return layer_grads


def reference(tokens, targets, w_in, w_out):
    tok_shards = tokens.reshape(SHARDS, TOK, D)
    tgt_shards = targets.reshape(SHARDS, TOK, D)

    def accumulate(running, shard_pair):
        grad_w_in, grad_w_out = shard_grads(shard_pair[0], shard_pair[1], w_in, w_out)
        return (running[0] + grad_w_in, running[1] + grad_w_out), None

    zero_acc = (jnp.zeros((LAYERS, D, FF), jnp.float32), jnp.zeros((LAYERS, FF, D), jnp.float32))
    totals = lax.scan(accumulate, zero_acc, (tok_shards, tgt_shards))[0]
    return totals[0], totals[1]
```

```python
import functools

import jax
import jax.numpy as jnp
from jax import lax
from jax.experimental import pallas as pl
from jax.experimental.pallas import tpu as pltpu
from jax.sharding import PartitionSpec as P

DATA_AXES = ('dy', 'dx')
ROW_CONTRACT = (((0,), (0,)), ((), ()))
COL_CONTRACT = (((1,), (1,)), ((), ()))


def forward_stack(tokens, w_in, w_out):
    hidden = tokens
    saved = []
    for layer in range(w_in.shape[0]):
        pre_act = jnp.dot(hidden, w_in[layer], preferred_element_type=jnp.float32).astype(jnp.bfloat16)
        post_act = jax.nn.gelu(pre_act.astype(jnp.float32)).astype(jnp.bfloat16)
        saved.append((hidden, pre_act, post_act))
        branch = jnp.dot(post_act, w_out[layer], preferred_element_type=jnp.float32)
        hidden = (hidden.astype(jnp.float32) + branch).astype(jnp.bfloat16)
    return hidden, saved


def layer_backward(grad_hid, hidden, pre_act, post_act, w_second):
    grad_w_out = lax.dot_general(post_act, grad_hid, ROW_CONTRACT, preferred_element_type=jnp.float32)
    grad_post = lax.dot_general(grad_hid, w_second, COL_CONTRACT, preferred_element_type=jnp.float32)
    gelu_vjp = jax.vjp(jax.nn.gelu, pre_act.astype(jnp.float32))[1]
    grad_pre = gelu_vjp(grad_post)[0].astype(jnp.bfloat16)
    grad_w_in = lax.dot_general(hidden, grad_pre, ROW_CONTRACT, preferred_element_type=jnp.float32)
    return grad_w_in, grad_w_out, grad_pre


def input_grad(grad_hid, grad_pre, w_first):
    through_w = lax.dot_general(grad_pre, w_first, COL_CONTRACT, preferred_element_type=jnp.float32)
    return (grad_hid.astype(jnp.float32) + through_w).astype(jnp.bfloat16)


def place(stacked, part, layer, layers):
    rows, cols = part.shape
    block = rows // 8

    def body(*refs):
        src, dst = refs[-2], refs[-1]
        dst[...] = src[...]

    slot = pl.BlockSpec((None, block, cols), lambda i: (layer, i, 0))
    specs = [pl.BlockSpec((block, cols), lambda i: (i, 0))]
    args = [part]
    aliases = {}
    if stacked is not None:
        specs = [pl.BlockSpec(memory_space=pl.ANY)] + specs
        args = [stacked] + args
        aliases = {0: 0}
    return pl.pallas_call(
        body,
        grid=(8,),
        in_specs=specs,
        out_specs=slot,
        out_shape=jax.ShapeDtypeStruct((layers, rows, cols), part.dtype),
        input_output_aliases=aliases,
        compiler_params=pltpu.CompilerParams(vmem_limit_bytes=32 << 20),
        cost_estimate=pl.CostEstimate(flops=20_000_000, bytes_accessed=8 * rows * cols, transcendentals=0),
        name=f'place_{layer}',
    )(*args)


def solution(mesh):
    def run(tokens, targets, w_in, w_out):
        inv_total = 1.0 / tokens.shape[0]

        def local_step(tok_local, tgt_local, w_first_all, w_second_all):
            final, saved = forward_stack(tok_local, w_first_all, w_second_all)
            grad_hid = ((final.astype(jnp.float32) - tgt_local.astype(jnp.float32)) * inv_total).astype(jnp.bfloat16)
            num_layers = w_first_all.shape[0]
            stacked_in = None
            stacked_out = None
            for layer in reversed(range(num_layers)):
                hidden, pre_act, post_act = saved[layer]
                grad_w_in, grad_w_out, grad_pre = layer_backward(grad_hid, hidden, pre_act, post_act, w_second_all[layer])
                own_out = lax.psum_scatter(grad_w_out, DATA_AXES, scatter_dimension=0, tiled=True)
                own_in = lax.psum_scatter(grad_w_in, DATA_AXES, scatter_dimension=0, tiled=True)
                full_out = lax.all_gather(own_out, DATA_AXES, axis=0, tiled=True)
                full_in = lax.all_gather(own_in, DATA_AXES, axis=0, tiled=True)
                stacked_out = place(stacked_out, full_out, layer, num_layers)
                stacked_in = place(stacked_in, full_in, layer, num_layers)
                if layer > 0:
                    grad_hid = input_grad(grad_hid, grad_pre, w_first_all[layer])
            return stacked_in, stacked_out

        data_spec = P(DATA_AXES, None)
        mapped = jax.shard_map(local_step, mesh=mesh, in_specs=(data_spec, data_spec, P(), P()), out_specs=(P(), P()), check_vma=False)
        return mapped(tokens, targets, w_in, w_out)

    return run
```

```python
import functools

import jax
import jax.numpy as jnp
from jax import lax
from jax.experimental import pallas as pl
from jax.experimental.pallas import tpu as pltpu
from jax.sharding import PartitionSpec as P

DATA_AXES = ('dy', 'dx')
MESH = pl.DeviceIdType.MESH
RING = 4
ROW_CONTRACT = (((0,), (0,)), ((), ()))
COL_CONTRACT = (((1,), (1,)), ((), ()))
F32, BF16 = jnp.float32, jnp.bfloat16


def local_pass(tokens, targets, w_in, w_out, inv_total):
    rows, dim = tokens.shape
    layers, _, hid = w_in.shape
    width = min(1024, hid)
    tiles = hid // width

    def body(tok, tgt, w1, w2, h_out, a_out, p_out, g_out, cur, acc, pre):
        step, tile = pl.program_id(0), pl.program_id(1)
        first, last = tile == 0, tile == tiles - 1

        def add(term):
            @pl.when(first)
            def _():
                acc[...] = term

            @pl.when(tile > 0)
            def _():
                acc[...] += term

        @pl.when((step == 0) & first)
        def _():
            cur[...] = tok[...]

        @pl.when(step < layers)
        def _():
            @pl.when(first)
            def _():
                h_out[...] = cur[...]

            pre_act = jnp.dot(cur[...], w1[...], preferred_element_type=F32).astype(BF16)
            pre[step, tile] = pre_act
            post_act = jax.nn.gelu(pre_act.astype(F32)).astype(BF16)
            a_out[...] = post_act
            add(jnp.dot(post_act, w2[...], preferred_element_type=F32))

            @pl.when(last)
            def _():
                cur[...] = (cur[...].astype(F32) + acc[...]).astype(BF16)

        @pl.when((step == layers - 1) & last)
        def _():
            cur[...] = ((cur[...].astype(F32) - tgt[...].astype(F32)) * inv_total).astype(BF16)

        @pl.when(step >= layers)
        def _():
            @pl.when(first)
            def _():
                g_out[...] = cur[...]

            grad_post = lax.dot_general(cur[...], w2[...], COL_CONTRACT, preferred_element_type=F32)
            pre_act = pre[2 * layers - 1 - step, tile].astype(F32)
            grad_pre = jax.vjp(jax.nn.gelu, pre_act)[1](grad_post)[0].astype(BF16)
            p_out[...] = grad_pre

            @pl.when(step < 2 * layers - 1)
            def _():
                add(lax.dot_general(grad_pre, w1[...], COL_CONTRACT, preferred_element_type=F32))

                @pl.when(last)
                def _():
                    cur[...] = (cur[...].astype(F32) + acc[...]).astype(BF16)

    top = layers - 1

    def layer_of(step):
        return jnp.where(step < layers, step, 2 * layers - 1 - step)

    def w1_at(step, tile):
        spare = step == 2 * layers - 1
        return jnp.where(spare, min(1, top), layer_of(step)), 0, jnp.where(spare, tiles - 1, tile)

    def fwd_at(step, tile):
        return jnp.minimum(step, top), 0, jnp.where(step < layers, tile, tiles - 1)

    def bwd_at(step, tile):
        return jnp.minimum(2 * layers - 1 - step, top), 0, jnp.where(step < layers, 0, tile)

    whole = pl.BlockSpec((rows, dim), lambda step, tile: (0, 0))
    return pl.pallas_call(
        body,
        grid=(2 * layers, tiles),
        in_specs=[
            whole,
            whole,
            pl.BlockSpec((None, dim, width), w1_at),
            pl.BlockSpec((None, width, dim), lambda step, tile: (layer_of(step), tile, 0)),
        ],
        out_specs=[
            pl.BlockSpec((None, rows, dim), lambda step, tile: (jnp.minimum(step, top), 0, 0)),
            pl.BlockSpec((None, rows, width), fwd_at),
            pl.BlockSpec((None, rows, width), bwd_at),
            pl.BlockSpec((None, rows, dim), lambda step, tile: (jnp.minimum(2 * layers - 1 - step, top), 0, 0)),
        ],
        out_shape=[
            jax.ShapeDtypeStruct((layers, rows, dim), BF16),
            jax.ShapeDtypeStruct((layers, rows, hid), BF16),
            jax.ShapeDtypeStruct((layers, rows, hid), BF16),
            jax.ShapeDtypeStruct((layers, rows, dim), BF16),
        ],
        scratch_shapes=[
            pltpu.VMEM((rows, dim), BF16),
            pltpu.VMEM((rows, dim), F32),
            pltpu.VMEM((layers, tiles, rows, width), BF16),
        ],
        compiler_params=pltpu.CompilerParams(vmem_limit_bytes=56 << 20, dimension_semantics=('arbitrary', 'arbitrary')),
        cost_estimate=pl.CostEstimate(
            flops=8 * layers * rows * dim * hid, bytes_accessed=8 * layers * dim * hid, transcendentals=2 * layers * rows * hid
        ),
        name='local_pass',
    )(tokens, targets, w_in, w_out)


OUT, IN = 0, 1
SHARES = ((6, 6, 4), (5, 5, 6))


class Reducer:
    def __init__(self, refs, layers, toks, dim, hid):
        (
            (self.h, self.a, self.p, self.g),
            (self.r_in, self.r_out, self.xh, self.xa, self.xp, self.xg),
            (self.lop, self.rop, self.wp, self.near, self.far),
            (self.rs_send, self.rs_recv, self.ag_send, self.ag_recv, self.pair_send, self.pair_recv, self.own_sem, self.load_sem),
            (self.x_send, self.x_recv),
        ) = refs
        self.layers, self.toks, self.half = layers, toks, hid // 2
        self.rows = (hid // 2, dim)
        cols = (dim, hid // 2)
        self.cut = []
        for kind in (OUT, IN):
            start, cuts = 0, []
            for share in SHARES[kind]:
                size = cols[kind] * share // 16
                cuts.append((start, size))
                start += size
            self.cut.append(cuts)
        dx = lax.axis_index('dx')
        self.core = lax.rem(dx, 2)
        self.at = (lax.axis_index('dy'), lax.rem(lax.div(dx, 2), RING), lax.div(dx, 2 * RING))

    def device(self, axis=None, shift=0, core=None):
        x, y, z = (lax.rem(c + shift, RING) if i == axis else c for i, c in enumerate(self.at))
        return x, (z * RING + y) * 2 + (self.core if core is None else core)

    def partner(self):
        return self.device(core=1 - self.core)

    def cols(self, kind, part):
        start, size = self.cut[kind][part]
        return pl.ds(start, size)

    def span(self, kind, part, phase, block, half=None):
        size = self.rows[kind] // RING
        base = 0
        for earlier in range(phase):
            base = base + self.at[(part + earlier) % 3] * size
            size //= RING
        row = base + lax.rem(self.at[(part + phase) % 3] + block, RING) * size
        if half is not None:
            size //= 2
            row = row + half * size
        return pl.multiple_of(row, size), size

    def result(self, kind, layer, part, row, size):
        start, width = self.cut[kind][part]
        if kind == OUT:
            return self.r_out.at[layer, pl.ds(pl.multiple_of(self.core * self.half + row, size), size), pl.ds(start, width)]
        col = pl.multiple_of(self.core * self.half + start, width if self.half % width == 0 else min(128, width))
        return self.r_in.at[layer, pl.ds(row, size), pl.ds(col, width)]


    def swap(self, kind, layer, j):
        theirs = pl.ds(pl.multiple_of((1 - self.core) * self.half, self.half), self.half)
        src, dst = (
            ((self.a.at[layer, :, theirs], self.xa.at[layer]), (self.g.at[layer], self.xg.at[layer])),
            ((self.h.at[layer], self.xh.at[layer]), (self.p.at[layer, :, theirs], self.xp.at[layer])),
        )[kind][j]
        return pltpu.make_async_remote_copy(
            src, dst, self.x_send.at[layer, kind, j], self.x_recv.at[layer, kind, j], device_id=self.partner(), device_id_type=MESH
        )

    def loads(self, kind, layer):
        mine = pl.ds(pl.multiple_of(self.core * self.half, self.half), self.half)
        own, other = pl.ds(0, self.toks), pl.ds(self.toks, self.toks)
        lop, rop, sem = self.lop[kind], self.rop[kind], self.load_sem[kind]
        first, second = (
            ((self.a.at[layer, :, mine], self.xa.at[layer]), (self.g.at[layer], self.xg.at[layer])),
            ((self.h.at[layer], self.xh.at[layer]), (self.p.at[layer, :, mine], self.xp.at[layer])),
        )[kind]
        return [
            pltpu.make_async_copy(first[0], lop.at[own], sem.at[0]),
            pltpu.make_async_copy(first[1], lop.at[other], sem.at[1]),
            pltpu.make_async_copy(second[0], rop.at[own], sem.at[2]),
            pltpu.make_async_copy(second[1], rop.at[other], sem.at[3]),
        ]

    def load(self, kind, layer):
        for j in range(2):
            self.swap(kind, layer, j).wait_recv()
        for copy in self.loads(kind, layer):
            copy.start()

    def product(self, kind, layer):
        for copy in self.loads(kind, layer):
            copy.wait()
        lop, rop, wp = self.lop[kind], self.rop[kind], self.wp[kind]
        block = min(256, self.rows[kind])

        def step(b, carry):
            rows = pl.ds(pl.multiple_of(b * block, block), block)
            wp[rows, :] = lax.dot_general(lop[:, rows], rop[...], ROW_CONTRACT, preferred_element_type=F32)
            return carry

        lax.fori_loop(0, self.rows[kind] // block, step, 0)


    def rs(self, kind, part, phase, step, way):
        if step == 0:
            row, size = self.span(kind, part, phase, 2, way)
            dst = self.near[kind][phase]
        else:
            row, size = self.span(kind, part, phase, 1 if way == 0 else 3)
            dst = self.far[kind][phase]
        cols = self.cols(kind, part)
        index = (part, phase, step, way)
        return pltpu.make_async_remote_copy(
            self.wp[kind].at[pl.ds(row, size), cols],
            dst.at[way, :, cols],
            self.rs_send[kind].at[index],
            self.rs_recv[kind].at[index],
            device_id=self.device((part + phase) % 3, 1 if way == 0 else 3),
            device_id_type=MESH,
        )

    def accumulate(self, kind, part, row, size, sources):
        cols = self.cols(kind, part)
        chunk = min(8, size)

        def step(i, carry):
            at = pl.multiple_of(i * chunk, chunk)
            here = pl.ds(pl.multiple_of(row + at, chunk), chunk)
            total = self.wp[kind][here, cols]
            for ref, slot in sources:
                total = total + ref[slot, pl.ds(at, chunk), cols]
            self.wp[kind][here, cols] = total
            return carry

        lax.fori_loop(0, size // chunk, step, 0)

    def reduce_1(self, kind, layer, phase):
        for part in range(3):
            for way in range(2):
                self.rs(kind, part, phase, 0, way).start()

    def reduce_2(self, kind, layer, phase):
        for part in range(3):
            for way in range(2):
                self.rs(kind, part, phase, 0, way).wait_recv()
                row, size = self.span(kind, part, phase, 1 if way == 0 else 3, way)
                self.accumulate(kind, part, row, size, [(self.near[kind][phase], way)])
                self.rs(kind, part, phase, 1, way).start()

    def reduce_3(self, kind, layer, phase):
        for part in range(3):
            for way in range(2):
                self.rs(kind, part, phase, 1, way).wait_recv()
            row, size = self.span(kind, part, phase, 0)
            self.accumulate(kind, part, row, size, [(self.far[kind][phase], 0), (self.far[kind][phase], 1)])
            for way in range(2):
                if phase < 2:
                    self.rs(kind, part, phase + 1, 0, way).start()
                else:
                    self.ag(kind, layer, part, 2, 0, way).start()
            if phase == 2:
                self.keep(kind, layer, part).start()


    def keep(self, kind, layer, part):
        row, size = self.span(kind, part, 2, 0)
        src = self.wp[kind].at[pl.ds(row, size), self.cols(kind, part)]
        return pltpu.make_async_copy(src, self.result(kind, layer, part, row, size), self.own_sem[kind].at[part])

    def ag(self, kind, layer, part, phase, step, way):
        if step == 0:
            row, size = self.span(kind, part, phase, 0)
        else:
            row, size = self.span(kind, part, phase, 3 if way == 0 else 1, way)
        dst = self.result(kind, layer, part, row, size)
        src = self.wp[kind].at[pl.ds(row, size), self.cols(kind, part)] if (phase, step) == (2, 0) else dst
        index = (part, phase, step, way)
        return pltpu.make_async_remote_copy(
            src,
            dst,
            self.ag_send[kind].at[index],
            self.ag_recv[kind].at[index],
            device_id=self.device((part + phase) % 3, 1 if way == 0 else 3),
            device_id_type=MESH,
        )

    def pair(self, kind, layer, part, j):
        block, half = ((0, None), (3, None), (1, None), (2, 0), (2, 1))[j]
        row, size = self.span(kind, part, 0, block, half)
        ref = self.result(kind, layer, part, row, size)
        return pltpu.make_async_remote_copy(
            ref, ref, self.pair_send[kind].at[part, j], self.pair_recv[kind].at[part, j], device_id=self.partner(), device_id_type=MESH
        )

    def gather_1(self, kind, layer, phase):
        for part in range(3):
            for way in range(2):
                self.ag(kind, layer, part, phase + 1, 1, way).wait_recv()
            if phase == 1:
                self.keep(kind, layer, part).wait()
            for way in range(2):
                self.ag(kind, layer, part, phase, 0, way).start()
            if phase == 0:
                self.pair(kind, layer, part, 0).start()

    def gather_2(self, kind, layer, phase):
        for part in range(3):
            for way in range(2):
                self.ag(kind, layer, part, phase, 0, way).wait_recv()
                self.ag(kind, layer, part, phase, 1, way).start()
                if phase == 0:
                    self.pair(kind, layer, part, 1 + way).start()

    def gather_3(self, kind, layer):
        for part in range(3):
            for way in range(2):
                self.ag(kind, layer, part, 0, 1, way).wait_recv()
                self.pair(kind, layer, part, 3 + way).start()

    def finish(self, kind, layer):
        for part in range(3):
            for phase in range(3):
                for step in range(2):
                    for way in range(2):
                        self.rs(kind, part, phase, step, way).wait_send()
                        self.ag(kind, layer, part, phase, step, way).wait_send()
            for j in range(5):
                self.pair(kind, layer, part, j).wait()


    def meet(self):
        barrier = pltpu.get_barrier_semaphore()
        others = [self.device(axis, shift) for axis in range(3) for shift in (1, 3)] + [self.partner()]
        for other in others:
            pl.semaphore_signal(barrier, inc=1, device_id=other, device_id_type=MESH)
        pl.semaphore_wait(barrier, len(others))

    def overlap(self, gathered, reduced, following):
        stages = (
            ('R', self.product),
            ('F', self.load),
            ('R', self.reduce_1, 0),
            ('G', self.gather_2, 2),
            ('G', self.gather_1, 1),
            ('R', self.reduce_2, 0),
            ('G', self.gather_2, 1),
            ('G', self.gather_1, 0),
            ('R', self.reduce_3, 0),
            ('R', self.reduce_2, 1),
            ('G', self.gather_2, 0),
            ('R', self.reduce_3, 1),
            ('R', self.reduce_2, 2),
            ('G', self.gather_3),
            ('R', self.reduce_3, 2),
            ('G', self.finish),
        )
        units = {'G': gathered, 'R': reduced, 'F': following}
        for whose, stage, *phase in stages:
            if units[whose] is not None:
                stage(*units[whose], *phase)

    def run(self):
        top = self.layers - 1
        self.meet()
        for layer in reversed(range(self.layers)):
            for kind in (OUT, IN):
                for j in range(2):
                    self.swap(kind, layer, j).start()
        self.load(OUT, top)
        self.overlap(None, (OUT, top), (IN, top))

        def step(i, carry):
            layer = top - i
            self.overlap((OUT, layer), (IN, layer), (OUT, layer - 1))
            self.overlap((IN, layer), (OUT, layer - 1), (IN, layer - 1))
            return carry

        lax.fori_loop(0, top, step, 0)
        self.overlap((OUT, 0), (IN, 0), None)
        self.overlap((IN, 0), None, None)
        for layer in reversed(range(self.layers)):
            for kind in (OUT, IN):
                for j in range(2):
                    self.swap(kind, layer, j).wait_send()


def reduce_grads(h, a, p, g):
    layers, toks, dim = h.shape
    hid = a.shape[-1]
    rows, cols = (hid // 2, dim), (dim, hid // 2)
    scratch = []
    for kind in (OUT, IN):
        block = rows[kind] // RING
        scratch += [
            pltpu.VMEM((2 * toks, rows[kind]), BF16),
            pltpu.VMEM((2 * toks, cols[kind]), BF16),
            pltpu.VMEM((rows[kind], cols[kind]), F32),
        ]
        for size in (block, block // RING, block // RING**2):
            scratch += [pltpu.VMEM((2, size // 2, cols[kind]), F32), pltpu.VMEM((2, size, cols[kind]), F32)]
    sems = [pltpu.SemaphoreType.DMA((3, 3, 2, 2))] * 4 + [pltpu.SemaphoreType.DMA((3, 5))] * 2
    sems += [pltpu.SemaphoreType.DMA((3,)), pltpu.SemaphoreType.DMA((4,))]
    scratch += sems * 2 + [pltpu.SemaphoreType.DMA((layers, 2, 2))] * 2

    def body(*refs):
        ins, outs, rest = refs[:4], refs[4:10], refs[10:]
        ops = rest[:9], rest[9:18]
        lop, rop, wp = ([o[i] for o in ops] for i in range(3))
        near, far = [o[3::2] for o in ops], [o[4::2] for o in ops]
        kinds = list(zip(rest[18:26], rest[26:34]))
        Reducer((ins, outs, (lop, rop, wp, near, far), kinds, rest[34:36]), layers, toks, dim, hid).run()

    anywhere = pl.BlockSpec(memory_space=pl.ANY)
    return pl.pallas_call(
        body,
        in_specs=[anywhere] * 4,
        out_specs=[anywhere] * 6,
        out_shape=[
            jax.ShapeDtypeStruct((layers, dim, hid), F32),
            jax.ShapeDtypeStruct((layers, hid, dim), F32),
            jax.ShapeDtypeStruct((layers, toks, dim), BF16),
            jax.ShapeDtypeStruct((layers, toks, hid // 2), BF16),
            jax.ShapeDtypeStruct((layers, toks, hid // 2), BF16),
            jax.ShapeDtypeStruct((layers, toks, dim), BF16),
        ],
        scratch_shapes=scratch,
        compiler_params=pltpu.CompilerParams(collective_id=1, has_side_effects=True, vmem_limit_bytes=60 << 20),
        cost_estimate=pl.CostEstimate(flops=4 * layers * toks * dim * hid, bytes_accessed=32 * layers * dim * hid, transcendentals=0),
        name='reduce_grads',
    )(h, a, p, g)[:2]


def solution(mesh):
    def run(tokens, targets, w_in, w_out):
        inv_total = 1.0 / tokens.shape[0]

        def local_step(tok_local, tgt_local, w_first_all, w_second_all):
            return reduce_grads(*local_pass(tok_local, tgt_local, w_first_all, w_second_all, inv_total))

        data_spec = P(DATA_AXES, None)
        mapped = jax.shard_map(local_step, mesh=mesh, in_specs=(data_spec, data_spec, P(), P()), out_specs=(P(), P()), check_vma=False)
        return mapped(tokens, targets, w_in, w_out)

    return run
```

```python
import functools

import jax
import jax.numpy as jnp
from jax import lax
from jax.experimental import pallas as pl
from jax.experimental.pallas import tpu as pltpu
from jax.sharding import PartitionSpec as P

DATA_AXES = ('dy', 'dx')
MESH = pl.DeviceIdType.MESH
RING = 4
ROW_CONTRACT = (((0,), (0,)), ((), ()))
COL_CONTRACT = (((1,), (1,)), ((), ()))
F32, BF16 = jnp.float32, jnp.bfloat16


def local_pass(tokens, targets, w_in, w_out, inv_total):
    rows, dim = tokens.shape
    layers, _, hid = w_in.shape
    width = min(1024, hid)
    tiles = hid // width

    def body(tok, tgt, w1, w2, h_out, a_out, p_out, g_out, cur, acc, pre):
        step, tile = pl.program_id(0), pl.program_id(1)
        first, last = tile == 0, tile == tiles - 1

        def add(term):
            @pl.when(first)
            def _():
                acc[...] = term

            @pl.when(tile > 0)
            def _():
                acc[...] += term

        @pl.when((step == 0) & first)
        def _():
            cur[...] = tok[...]

        @pl.when(step < layers)
        def _():
            @pl.when(first)
            def _():
                h_out[...] = cur[...]

            pre_act = jnp.dot(cur[...], w1[...], preferred_element_type=F32).astype(BF16)
            pre[step, tile] = pre_act
            post_act = jax.nn.gelu(pre_act.astype(F32)).astype(BF16)
            a_out[...] = post_act
            add(jnp.dot(post_act, w2[...], preferred_element_type=F32))

            @pl.when(last)
            def _():
                cur[...] = (cur[...].astype(F32) + acc[...]).astype(BF16)

        @pl.when((step == layers - 1) & last)
        def _():
            cur[...] = ((cur[...].astype(F32) - tgt[...].astype(F32)) * inv_total).astype(BF16)

        @pl.when(step >= layers)
        def _():
            @pl.when(first)
            def _():
                g_out[...] = cur[...]

            grad_post = lax.dot_general(cur[...], w2[...], COL_CONTRACT, preferred_element_type=F32)
            pre_act = pre[2 * layers - 1 - step, tile].astype(F32)
            grad_pre = jax.vjp(jax.nn.gelu, pre_act)[1](grad_post)[0].astype(BF16)
            p_out[...] = grad_pre

            @pl.when(step < 2 * layers - 1)
            def _():
                add(lax.dot_general(grad_pre, w1[...], COL_CONTRACT, preferred_element_type=F32))

                @pl.when(last)
                def _():
                    cur[...] = (cur[...].astype(F32) + acc[...]).astype(BF16)

    top = layers - 1

    def layer_of(step):
        return jnp.where(step < layers, step, 2 * layers - 1 - step)

    def w1_at(step, tile):
        spare = step == 2 * layers - 1
        return jnp.where(spare, min(1, top), layer_of(step)), 0, jnp.where(spare, tiles - 1, tile)

    def fwd_at(step, tile):
        return jnp.minimum(step, top), 0, jnp.where(step < layers, tile, tiles - 1)

    def bwd_at(step, tile):
        return jnp.minimum(2 * layers - 1 - step, top), 0, jnp.where(step < layers, 0, tile)

    whole = pl.BlockSpec((rows, dim), lambda step, tile: (0, 0))
    return pl.pallas_call(
        body,
        grid=(2 * layers, tiles),
        in_specs=[
            whole,
            whole,
            pl.BlockSpec((None, dim, width), w1_at),
            pl.BlockSpec((None, width, dim), lambda step, tile: (layer_of(step), tile, 0)),
        ],
        out_specs=[
            pl.BlockSpec((None, rows, dim), lambda step, tile: (jnp.minimum(step, top), 0, 0)),
            pl.BlockSpec((None, rows, width), fwd_at),
            pl.BlockSpec((None, rows, width), bwd_at),
            pl.BlockSpec((None, rows, dim), lambda step, tile: (jnp.minimum(2 * layers - 1 - step, top), 0, 0)),
        ],
        out_shape=[
            jax.ShapeDtypeStruct((layers, rows, dim), BF16),
            jax.ShapeDtypeStruct((layers, rows, hid), BF16),
            jax.ShapeDtypeStruct((layers, rows, hid), BF16),
            jax.ShapeDtypeStruct((layers, rows, dim), BF16),
        ],
        scratch_shapes=[
            pltpu.VMEM((rows, dim), BF16),
            pltpu.VMEM((rows, dim), F32),
            pltpu.VMEM((layers, tiles, rows, width), BF16),
        ],
        compiler_params=pltpu.CompilerParams(vmem_limit_bytes=56 << 20, dimension_semantics=('arbitrary', 'arbitrary')),
        cost_estimate=pl.CostEstimate(
            flops=8 * layers * rows * dim * hid, bytes_accessed=8 * layers * dim * hid, transcendentals=2 * layers * rows * hid
        ),
        name='local_pass',
    )(tokens, targets, w_in, w_out)


OUT, IN = 0, 1
STAGES = (
    ('swap_1', 0),
    ('swap_2', 2.16),
    ('swap_3', 3.02),
    ('load', 3.21),
    ('product', 3.64),
    ('reduce_2', 4.27),
    ('reduce_3', 6.08),
    ('reduce_4', 6.87),
    ('reduce_5', 7.3),
    ('gather_1', 7.95),
    ('gather_2', 8.64),
    ('gather_3', 9.09),
    ('gather_4', 10.02),
    ('gather_5', 11.68),
    ('gather_6', 14.27),
)


def once(method):
    @functools.wraps(method)
    def get(self, *args):
        key = method.__name__, args
        if key not in self.memo:
            self.memo[key] = method(self, *args)
        return self.memo[key]

    return get


class Reducer:
    def __init__(self, ins, outs, scratch, layers, toks, dim, hid):
        self.h, self.a, self.p, self.g = ins
        self.r_in, self.r_out, self.fx, self.sx, self.tx = outs
        self.fbuf, self.sbuf, self.wp, self.near, self.far, self.sems, self.load_sem, self.own_sem = scratch
        self.layers, self.toks, self.dim, self.hid = layers, toks, dim, hid
        self.memo = {}
        self.piece, self.edge = hid // 8, dim // 2
        dx = lax.axis_index('dx')
        self.core = lax.rem(dx, 2)
        self.at = (lax.axis_index('dy'), lax.rem(lax.div(dx, 2), RING), lax.div(dx, 2 * RING))

    def kind(self, unit):
        return unit % 2

    def layer(self, unit):
        return self.layers - 1 - unit // 2

    def axis(self, unit, k):
        return (unit + k) % 3

    @once
    def ring(self, axis, shift):
        return lax.rem(self.at[axis] + shift, RING)

    @once
    def chip(self, axis, shift):
        x, y, z = (self.ring(i, shift) if i == axis else c for i, c in enumerate(self.at))
        return x, (z * RING + y) * 2

    @once
    def device(self, axis, shift, core=None):
        x, rest = self.chip(axis, shift)
        return x, rest + (self.core if core is None else core)

    @once
    def partner(self):
        x, rest = self.chip(None, 0)
        return x, rest + (1 - self.core)

    def copy(self, unit, index, src, dst, device, recv_index=None):
        recv = index if recv_index is None else recv_index
        return pltpu.make_async_remote_copy(
            src, dst, self.sems.at[0, unit, index], self.sems.at[1, unit, recv], device_id=device, device_id_type=MESH
        )


    def full(self, unit):
        return (self.g, self.h)[self.kind(unit)].at[self.layer(unit)]

    def cut(self, unit, ring, core, rows=None):
        cols = pl.ds(pl.multiple_of((core * RING + ring) * self.piece, self.piece), self.piece)
        ref = (self.a, self.p)[self.kind(unit)]
        return ref.at[self.layer(unit), pl.ds(*(rows or (0, self.toks))), cols]

    def half(self, way):
        return way * (self.toks // 2), self.toks // 2

    @once
    def slot(self, unit, shift, other=0):
        return self.ring(self.axis(unit, 0), shift) * 2 + (1 - self.core if other else self.core)

    @once
    def full_out(self, unit, way):
        ref = self.fx.at[unit, self.slot(unit, 0)]
        return self.copy(unit, way, self.full(unit), ref, self.device(self.axis(unit, 0), 1 + 2 * way))

    @once
    def cut_out(self, unit, way, core, source=None):
        axis, shift = self.axis(unit, 0), 1 + 2 * way
        src = self.cut(unit, self.ring(axis, shift), core)
        dst = self.sx.at[unit, self.slot(unit, 0)]
        recv = 2 + 2 * way + (self.core if source is None else source)
        return self.copy(unit, 2 + 2 * way + core, src, dst, self.device(axis, shift, core), recv)

    @once
    def transit_out(self, unit, way, core):
        axis = self.axis(unit, 0)
        src = self.cut(unit, self.ring(axis, 2), core, self.half(way))
        return self.copy(unit, 6 + 2 * way + core, src, self.tx.at[unit, way, core], self.device(axis, 1 + 2 * way))

    @once
    def full_on(self, unit, way):
        ref = self.fx.at[unit, self.slot(unit, 3 - 2 * way), pl.ds(*self.half(way))]
        return self.copy(unit, 10 + way, ref, ref, self.device(self.axis(unit, 0), 1 + 2 * way))

    @once
    def transit_on(self, unit, way, core, source=None):
        dst = self.sx.at[unit, self.slot(unit, 3 - 2 * way), pl.ds(*self.half(way))]
        device = self.device(self.axis(unit, 0), 1 + 2 * way, core)
        recv = 12 + 2 * way + (self.core if source is None else source)
        return self.copy(unit, 12 + 2 * way + core, self.tx.at[unit, way, core], dst, device, recv)

    @once
    def full_pair(self, unit, j):
        ref = self.fx.at[unit, self.slot(unit, (0, 3, 1, 2)[j])]
        return self.copy(unit, 16 + j, self.full(unit) if j == 0 else ref, ref, self.partner())

    @once
    def cut_pair(self, unit):
        src = self.cut(unit, self.at[self.axis(unit, 0)], 1 - self.core)
        dst = self.sx.at[unit, self.slot(unit, 0)]
        return self.copy(unit, 20, src, dst, self.partner())

    def swap_1(self, unit):
        for way in range(2):
            self.full_out(unit, way).start()
            for core in range(2):
                self.transit_out(unit, way, core).start()
        self.full_pair(unit, 0).start()
        self.cut_pair(unit).start()
        for way in range(2):
            for core in range(2):
                self.cut_out(unit, way, core).start()

    def swap_2(self, unit):
        for way in range(2):
            self.full_out(unit, way).wait_recv()
            self.full_on(unit, way).start()
            self.full_pair(unit, 1 + way).start()
        for way in range(2):
            for core in range(2):
                self.transit_out(unit, way, core).wait_recv()
                self.transit_on(unit, way, core).start()

    def swap_3(self, unit):
        for way in range(2):
            self.full_on(unit, way).wait_recv()
        self.full_pair(unit, 3).start()


    @once
    def loads(self, unit):
        copies = []
        for j in range(8):
            rows = pl.ds(j * self.toks, self.toks)
            if j == 0:
                full, cut = self.full(unit), self.cut(unit, self.at[self.axis(unit, 0)], self.core)
            else:
                slot = self.slot(unit, j // 2, j % 2)
                full, cut = self.fx.at[unit, slot], self.sx.at[unit, slot]
            parity = unit % 2
            copies.append(pltpu.make_async_copy(full, self.fbuf.at[parity, rows], self.load_sem.at[parity, 0, j]))
            copies.append(pltpu.make_async_copy(cut, self.sbuf.at[parity, rows], self.load_sem.at[parity, 1, j]))
        return copies

    def load(self, unit):
        for j in range(4):
            self.full_pair(unit, j).wait_recv()
        self.cut_pair(unit).wait_recv()
        for way in range(2):
            for source in range(2):
                self.cut_out(unit, way, 0, source).wait_recv()
                self.transit_on(unit, way, 0, source).wait_recv()
        for copy in self.loads(unit):
            copy.start()

    def product(self, unit):
        for copy in self.loads(unit):
            copy.wait()
        fbuf, sbuf, wp, edge = self.fbuf.at[unit % 2], self.sbuf.at[unit % 2], self.wp.at[unit], self.edge
        block = edge // 2

        def step(b, carry):
            rows = pl.ds(pl.multiple_of(b * block, block), block)
            if self.kind(unit) == OUT:
                for part in range(2):
                    cols = pl.ds(part * edge, edge)
                    wp[part, rows] = lax.dot_general(sbuf[:, rows], fbuf[:, cols], ROW_CONTRACT, preferred_element_type=F32)
            else:
                term = lax.dot_general(fbuf[:, rows], sbuf[...], ROW_CONTRACT, preferred_element_type=F32)
                wp[lax.div(b, 2), pl.ds(pl.multiple_of(lax.rem(b, 2) * block, block), block)] = term
            return carry

        lax.fori_loop(0, 2 if self.kind(unit) == OUT else 4, step, 0)
        for part in range(2):
            for way in range(2):
                self.rs(unit, part, 0, 0, way).start()


    def rs_axis(self, unit, part, phase):
        return self.axis(unit, 1 + (part + phase) % 2)

    @once
    def span(self, unit, part, phase, block, half=None):
        size = self.edge // RING
        base = 0
        if phase:
            base = self.at[self.rs_axis(unit, part, 0)] * size
            size //= RING
        row = base + self.ring(self.rs_axis(unit, part, phase), block) * size
        if half is not None:
            size //= 2
            row = row + half * size
        return pl.multiple_of(row, size), size

    @once
    def rs(self, unit, part, phase, step, way):
        if step == 0:
            row, size = self.span(unit, part, phase, 2, way)
            dst = self.near[phase]
        else:
            row, size = self.span(unit, part, phase, 1 + 2 * way)
            dst = self.far[phase]
        index = 21 + ((part * 2 + phase) * 2 + step) * 2 + way
        src = self.wp.at[unit, part, pl.ds(row, size)]
        return self.copy(unit, index, src, dst.at[unit, part, way], self.device(self.rs_axis(unit, part, phase), 1 + 2 * way))

    def accumulate(self, unit, part, row, size, sources):
        chunk = min(16, size)

        def step(i, carry):
            at = pl.multiple_of(i * chunk, chunk)
            here = pl.ds(pl.multiple_of(row + at, chunk), chunk)
            total = self.wp[unit, part, here]
            for ref, way in sources:
                total = total + ref[unit, part, way, pl.ds(at, chunk)]
            self.wp[unit, part, here] = total
            return carry

        lax.fori_loop(0, size // chunk, step, 0)

    def reduce_near(self, unit, phase):
        for part in range(2):
            for way in range(2):
                self.rs(unit, part, phase, 0, way).wait_recv()
                row, size = self.span(unit, part, phase, 1 + 2 * way, way)
                self.accumulate(unit, part, row, size, [(self.near[phase], way)])
                self.rs(unit, part, phase, 1, way).start()

    def reduce_far(self, unit, phase):
        for part in range(2):
            for way in range(2):
                self.rs(unit, part, phase, 1, way).wait_recv()
            row, size = self.span(unit, part, phase, 0)
            self.accumulate(unit, part, row, size, [(self.far[phase], 0), (self.far[phase], 1)])
            for way in range(2):
                if phase == 0:
                    self.rs(unit, part, 1, 0, way).start()
                else:
                    self.ag(unit, part, 0, 0, way).start()
            if phase == 1:
                self.keep(unit, part).start()

    def reduce_2(self, unit):
        self.reduce_near(unit, 0)

    def reduce_3(self, unit):
        self.reduce_far(unit, 0)

    def reduce_4(self, unit):
        self.reduce_near(unit, 1)

    def reduce_5(self, unit):
        self.reduce_far(unit, 1)


    def result(self, unit, part, row, size, shift=None):
        layer, edge, piece = self.layer(unit), self.edge, self.piece
        if shift is None:
            first, count = self.core * RING, RING
        else:
            first, count = self.core * RING + self.ring(self.axis(unit, 0), shift), 1
        if self.kind(unit) == OUT:
            return self.r_out.at[layer, pl.ds(first, count), pl.ds(row, size), pl.ds(part * edge, edge)]
        cols = pl.ds(pl.multiple_of(first * piece, piece), count * piece)
        return self.r_in.at[layer, pl.ds(pl.multiple_of(part * edge + row, size), size), cols]

    def shard(self, unit, part):
        row, size = self.span(unit, part, 1, 0)
        return self.wp.at[unit, pl.ds(part, 1), pl.ds(row, size)] if self.kind(unit) == OUT else self.wp.at[unit, part, pl.ds(row, size)]

    @once
    def keep(self, unit, part):
        return pltpu.make_async_copy(
            self.shard(unit, part), self.result(unit, part, *self.span(unit, part, 1, 0), 0), self.own_sem.at[unit, part]
        )

    @once
    def ag(self, unit, part, phase, step, way):
        if phase == 0:
            axis = self.axis(unit, 0)
            row, size = self.span(unit, part, 1, 0)
            if step:
                size //= 2
                row = row + way * size
            dst = self.result(unit, part, pl.multiple_of(row, size), size, 3 - 2 * way if step else 0)
            src = dst if step else self.shard(unit, part)
        else:
            axis = self.rs_axis(unit, part, 2 - phase)
            row, size = self.span(unit, part, 2 - phase, 3 - 2 * way, way) if step else self.span(unit, part, 2 - phase, 0)
            src = dst = self.result(unit, part, row, size)
        index = 37 + ((part * 3 + phase) * 2 + step) * 2 + way
        return self.copy(unit, index, src, dst, self.device(axis, 1 + 2 * way))

    @once
    def pair(self, unit, part, j):
        block, half = ((0, None), (3, None), (1, None), (2, 0), (2, 1))[j]
        ref = self.result(unit, part, *self.span(unit, part, 0, block, half))
        return self.copy(unit, 61 + part * 5 + j, ref, ref, self.partner())

    def gather_on(self, unit, phase):
        for part in range(2):
            for way in range(2):
                self.ag(unit, part, phase, 0, way).wait_recv()
                self.ag(unit, part, phase, 1, way).start()
                if phase == 2:
                    self.pair(unit, part, 1 + way).start()

    def gather_next(self, unit, phase):
        for part in range(2):
            for way in range(2):
                self.ag(unit, part, phase - 1, 1, way).wait_recv()
            if phase == 1:
                self.keep(unit, part).wait()
            for way in range(2):
                self.ag(unit, part, phase, 0, way).start()
            if phase == 2:
                self.pair(unit, part, 0).start()

    def gather_1(self, unit):
        self.gather_on(unit, 0)

    def gather_2(self, unit):
        self.gather_next(unit, 1)

    def gather_3(self, unit):
        self.gather_on(unit, 1)

    def gather_4(self, unit):
        self.gather_next(unit, 2)

    def gather_5(self, unit):
        self.gather_on(unit, 2)

    def gather_6(self, unit):
        for part in range(2):
            for way in range(2):
                self.ag(unit, part, 2, 1, way).wait_recv()
                self.pair(unit, part, 3 + way).start()

    def finish(self, unit):
        for part in range(2):
            for j in range(5):
                self.pair(unit, part, j).wait()
            for way in range(2):
                for step in range(2):
                    for phase in range(2):
                        self.rs(unit, part, phase, step, way).wait_send()
                    for phase in range(3):
                        self.ag(unit, part, phase, step, way).wait_send()
        for way in range(2):
            self.full_out(unit, way).wait_send()
            self.full_on(unit, way).wait_send()
            for core in range(2):
                self.cut_out(unit, way, core).wait_send()
                self.transit_out(unit, way, core).wait_send()
                self.transit_on(unit, way, core).wait_send()
        for j in range(4):
            self.full_pair(unit, j).wait_send()
        self.cut_pair(unit).wait_send()

    def meet(self):
        barrier = pltpu.get_barrier_semaphore()
        others = [self.device(axis, shift, core) for axis in range(3) for shift in (1, 3) for core in range(2)]
        others.append(self.partner())
        for other in others:
            pl.semaphore_signal(barrier, inc=1, device_id=other, device_id_type=MESH)
        pl.semaphore_wait(barrier, len(others))

    def run(self):
        self.meet()
        units = range(2 * self.layers)
        order = sorted((unit + offset, k, unit) for unit in units for k, (_, offset) in enumerate(STAGES))
        for _, k, unit in order:
            getattr(self, STAGES[k][0])(unit)
        for unit in units:
            self.finish(unit)


def reduce_grads(h, a, p, g):
    layers, toks, dim = h.shape
    hid = a.shape[-1]
    units, edge, piece = 2 * layers, dim // 2, hid // 8
    assert edge == piece
    block, small = edge // RING, edge // RING**2

    def body(*refs):
        near, far = (refs[12], refs[14]), (refs[13], refs[15])
        Reducer(refs[:4], refs[4:9], (*refs[9:12], near, far, *refs[16:]), layers, toks, dim, hid).run()

    anywhere = pl.BlockSpec(memory_space=pl.ANY)
    grad_in, grad_out, *_ = pl.pallas_call(
        body,
        in_specs=[anywhere] * 4,
        out_specs=[anywhere] * 5,
        out_shape=[
            jax.ShapeDtypeStruct((layers, dim, hid), F32),
            jax.ShapeDtypeStruct((layers, 8, piece, dim), F32),
            jax.ShapeDtypeStruct((units, 8, toks, dim), BF16),
            jax.ShapeDtypeStruct((units, 8, toks, piece), BF16),
            jax.ShapeDtypeStruct((units, 2, 2, toks // 2, piece), BF16),
        ],
        scratch_shapes=[
            pltpu.VMEM((2, 8 * toks, dim), BF16),
            pltpu.VMEM((2, 8 * toks, piece), BF16),
            pltpu.VMEM((units, 2, edge, edge), F32),
            pltpu.VMEM((units, 2, 2, block // 2, edge), F32),
            pltpu.VMEM((units, 2, 2, block, edge), F32),
            pltpu.VMEM((units, 2, 2, small // 2, edge), F32),
            pltpu.VMEM((units, 2, 2, small, edge), F32),
            pltpu.SemaphoreType.DMA((2, units, 71)),
            pltpu.SemaphoreType.DMA((2, 2, 8)),
            pltpu.SemaphoreType.DMA((units, 2)),
        ],
        compiler_params=pltpu.CompilerParams(collective_id=1, has_side_effects=True, vmem_limit_bytes=60 << 20),
        cost_estimate=pl.CostEstimate(flops=4 * layers * toks * dim * hid, bytes_accessed=32 * layers * dim * hid, transcendentals=0),
        name='reduce_grads',
    )(h, a, p, g)
    return grad_in, grad_out.reshape(layers, hid, dim)


def solution(mesh):
    def run(tokens, targets, w_in, w_out):
        inv_total = 1.0 / tokens.shape[0]

        def local_step(tok_local, tgt_local, w_first_all, w_second_all):
            return reduce_grads(*local_pass(tok_local, tgt_local, w_first_all, w_second_all, inv_total))

        data_spec = P(DATA_AXES, None)
        mapped = jax.shard_map(local_step, mesh=mesh, in_specs=(data_spec, data_spec, P(), P()), out_specs=(P(), P()), check_vma=False)
        return mapped(tokens, targets, w_in, w_out)

    return run
```

```python
import functools

import jax
import jax.numpy as jnp
from jax import lax
from jax.experimental import pallas as pl
from jax.experimental.pallas import tpu as pltpu
from jax.sharding import PartitionSpec as P

DATA_AXES = ('dy', 'dx')
MESH = pl.DeviceIdType.MESH
RING = 4
ROW_CONTRACT = (((0,), (0,)), ((), ()))
COL_CONTRACT = (((1,), (1,)), ((), ()))
F32, BF16 = jnp.float32, jnp.bfloat16


OUT, IN = 0, 1
HELD = 6
STAGES = (
    'forward',
    'backward',
    'swap_full',
    'swap_cut',
    'full_2',
    'cut_2',
    'full_3',
    'load',
    'product',
    'reduce_2',
    'reduce_3',
    'reduce_4',
    'reduce_5',
    'gather_1',
    'gather_2',
    'gather_3',
    'gather_4',
    'gather_5',
    'gather_6',
)
ORDER = (
    27, 0, 36, 1, 34, 25, 23, 2, 21, 32, 3, 20, 54, 13, 31, 22, 30, 45, 52, 12,
    41, 50, 40, 51, 43, 11, 35, 24, 10, 60, 33, 61, 70, 42, 63, 80, 71, 37, 81, 90,
    53, 55, 91, 26, 62, 72, 65, 82, 73, 100, 44, 101, 110, 83, 47, 120, 64, 111, 93, 74,
    130, 140, 46, 84, 121, 75, 103, 56, 150, 94, 113, 131, 57, 85, 160, 95, 141, 123, 66, 76,
    86, 67, 77, 92, 87, 104, 151, 97, 133, 96, 107, 102, 143, 114, 117, 105, 112, 161, 124, 134,
    122, 127, 106, 137, 147, 115, 132, 171, 157, 116, 142, 153, 125, 170, 126, 144, 135, 136, 152, 163,
    167, 162, 154, 180, 145, 173, 172, 155, 146, 164, 181, 165, 183, 182, 156, 177, 166, 174, 175, 187,
    176, 184, 185, 186,
)


def once(method):
    @functools.wraps(method)
    def get(self, *args):
        key = method.__name__, args
        if key not in self.memo:
            self.memo[key] = method(self, *args)
        return self.memo[key]

    return get


class Reducer:
    def __init__(self, ins, outs, scratch, layers, toks, dim, hid, inv_total):
        self.tokens, self.targets, self.w_in, self.w_out = ins
        self.r_in, self.r_out, self.fx, self.sx, self.tx, self.h, self.a, self.p, self.g = outs
        self.fbuf, self.sbuf, self.wp, self.near, self.far, self.sems, self.load_sem, self.own_sem, *local = scratch
        self.cur, self.acc, self.pre, self.wide, self.w1, self.w2, self.w_sem, self.out_sem = local
        self.tile = self.w1.shape[-1]
        self.tiles, self.slots = hid // self.tile, self.w1.shape[0]
        self.layers, self.toks, self.dim, self.hid = layers, toks, dim, hid
        self.memo = {}
        self.inv_total = inv_total
        self.piece, self.edge = hid // 8, dim // 2
        dx = lax.axis_index('dx')
        self.core = lax.rem(dx, 2)
        self.at = (lax.axis_index('dy'), lax.rem(lax.div(dx, 2), RING), lax.div(dx, 2 * RING))

    def kind(self, unit):
        return unit % 2

    def layer(self, unit):
        return self.layers - 1 - unit // 2

    def axis(self, unit, k):
        return (unit + k) % 3

    @once
    def ring(self, axis, shift):
        return lax.rem(self.at[axis] + shift, RING)

    @once
    def chip(self, axis, shift):
        x, y, z = (self.ring(i, shift) if i == axis else c for i, c in enumerate(self.at))
        return x, (z * RING + y) * 2

    @once
    def device(self, axis, shift, core=None):
        x, rest = self.chip(axis, shift)
        return x, rest + (self.core if core is None else core)

    @once
    def partner(self):
        x, rest = self.chip(None, 0)
        return x, rest + (1 - self.core)

    def copy(self, unit, index, src, dst, device, recv_index=None):
        recv = index if recv_index is None else recv_index
        return pltpu.make_async_remote_copy(
            src, dst, self.sems.at[0, unit, index], self.sems.at[1, unit, recv], device_id=device, device_id_type=MESH
        )


    def move(self, src, dst):
        return pltpu.make_async_copy(src, dst, self.out_sem.at[self.tiles])

    def fetch(self, layer, tile, first):
        part, slot = pl.ds(pl.multiple_of(tile * self.tile, self.tile), self.tile), lax.rem(tile, self.slots)
        copies = [pltpu.make_async_copy(self.w_out.at[layer, part], self.w2.at[slot], self.w_sem.at[slot, 1])]
        if first:
            copies.append(pltpu.make_async_copy(self.w_in.at[layer, :, part], self.w1.at[slot], self.w_sem.at[slot, 0]))
        return copies

    def ahead(self, layer, first):
        for tile in range(self.slots - 1):
            for copy in self.fetch(layer, tile, first):
                copy.start()

    def over_tiles(self, layer, first, following, work, out):
        tiles = self.tiles

        def result(tile):
            part = pl.ds(pl.multiple_of(tile * self.tile, self.tile), self.tile)
            return part, pltpu.make_async_copy(self.wide.at[:, part], out.at[layer, :, part], self.out_sem.at[tile])

        def step(tile, carry):
            for copy in self.fetch(layer, tile, first):
                copy.wait()
            later = tile + self.slots - 1

            @pl.when(later < tiles)
            def _():
                for copy in self.fetch(layer, later, first):
                    copy.start()

            if following is not None:

                @pl.when(later >= tiles)
                def _():
                    for copy in self.fetch(following[0], later - tiles, following[1]):
                        copy.start()

            part, copy = result(tile)
            work(lax.rem(tile, self.slots), part)
            copy.start()
            return carry

        lax.fori_loop(0, tiles, step, 0)

        def wait(tile, carry):
            result(tile)[1].wait()
            return carry

        lax.fori_loop(0, tiles, wait, 0)

    def forward(self, layer):
        top = self.layers - 1

        def work(slot, part):
            pre_act = jnp.dot(self.cur[:, :], self.w1[slot], preferred_element_type=F32).astype(BF16)
            self.pre[layer, :, part] = pre_act
            post_act = jax.nn.gelu(pre_act.astype(F32)).astype(BF16)
            self.wide[:, part] = post_act
            self.acc[:, :] += jnp.dot(post_act, self.w2[slot], preferred_element_type=F32)

        self.acc[:, :] = self.cur[:, :].astype(F32)
        following = (layer + 1, True) if layer < top else (top, top > 0)
        self.over_tiles(layer, True, following, work, self.a)
        self.cur[:, :] = self.acc[:, :].astype(BF16)
        if layer == top:
            copy = self.move(self.targets, self.wide.at[:, pl.ds(0, self.dim)])
            copy.start()
            copy.wait()
            gap = self.cur[:, :].astype(F32) - self.wide[:, pl.ds(0, self.dim)].astype(F32)
            self.cur[:, :] = (gap * self.inv_total).astype(BF16)
        copy = self.move(self.cur, self.h.at[layer + 1] if layer < top else self.g.at[top])
        copy.start()
        copy.wait()

    def backward(self, layer):
        def work(slot, part):
            grad_post = lax.dot_general(self.cur[:, :], self.w2[slot], COL_CONTRACT, preferred_element_type=F32)
            pre_act = self.pre[layer, :, part].astype(F32)
            grad_pre = jax.vjp(jax.nn.gelu, pre_act)[1](grad_post)[0].astype(BF16)
            self.wide[:, part] = grad_pre
            if layer > 0:
                self.acc[:, :] += lax.dot_general(grad_pre, self.w1[slot], COL_CONTRACT, preferred_element_type=F32)

        if layer > 0:
            self.acc[:, :] = self.cur[:, :].astype(F32)
        self.over_tiles(layer, layer > 0, (layer - 1, layer > 1) if layer > 0 else None, work, self.p)
        if layer > 0:
            self.cur[:, :] = self.acc[:, :].astype(BF16)
            copy = self.move(self.cur, self.g.at[layer - 1])
            copy.start()
            copy.wait()


    def full(self, unit):
        layer = self.layer(unit)
        if self.kind(unit) == IN and layer == 0:
            return self.tokens
        return (self.g, self.h)[self.kind(unit)].at[layer]

    def cut(self, unit, ring, core, rows=None):
        cols = pl.ds(pl.multiple_of((core * RING + ring) * self.piece, self.piece), self.piece)
        ref = (self.a, self.p)[self.kind(unit)]
        return ref.at[self.layer(unit), pl.ds(*(rows or (0, self.toks))), cols]

    def side(self, way):
        return 1 + 2 * way

    def back(self, way):
        return RING - self.side(way)

    def half(self, way):
        return way * (self.toks // 2), self.toks // 2

    @once
    def slot(self, unit, shift, other=0):
        return self.ring(self.axis(unit, 0), shift) * 2 + (1 - self.core if other else self.core)

    @once
    def full_out(self, unit, way):
        ref = self.fx.at[unit, self.slot(unit, 0)]
        return self.copy(unit, way, self.full(unit), ref, self.device(self.axis(unit, 0), self.side(way)))

    @once
    def cut_out(self, unit, way, core, source=None):
        axis, shift = self.axis(unit, 0), self.side(way)
        src = self.cut(unit, self.ring(axis, shift), core)
        dst = self.sx.at[unit, self.slot(unit, 0)]
        recv = 2 + 2 * way + (self.core if source is None else source)
        return self.copy(unit, 2 + 2 * way + core, src, dst, self.device(axis, shift, core), recv)

    @once
    def transit_out(self, unit, way, core):
        axis = self.axis(unit, 0)
        src = self.cut(unit, self.ring(axis, 2), core, self.half(way))
        return self.copy(unit, 6 + 2 * way + core, src, self.tx.at[unit, way, core], self.device(axis, self.side(way)))

    @once
    def full_on(self, unit, way):
        ref = self.fx.at[unit, self.slot(unit, self.back(way)), pl.ds(*self.half(way))]
        return self.copy(unit, 10 + way, ref, ref, self.device(self.axis(unit, 0), self.side(way)))

    @once
    def transit_on(self, unit, way, core, source=None):
        dst = self.sx.at[unit, self.slot(unit, self.back(way)), pl.ds(*self.half(way))]
        device = self.device(self.axis(unit, 0), self.side(way), core)
        recv = 12 + 2 * way + (self.core if source is None else source)
        return self.copy(unit, 12 + 2 * way + core, self.tx.at[unit, way, core], dst, device, recv)

    @once
    def full_pair(self, unit, j):
        ref = self.fx.at[unit, self.slot(unit, (0, 3, 1, 2)[j])]
        return self.copy(unit, 16 + j, self.full(unit) if j == 0 else ref, ref, self.partner())

    @once
    def cut_pair(self, unit):
        src = self.cut(unit, self.at[self.axis(unit, 0)], 1 - self.core)
        dst = self.sx.at[unit, self.slot(unit, 0)]
        return self.copy(unit, 20, src, dst, self.partner())

    def swap_full(self, unit):
        for way in range(2):
            self.full_out(unit, way).start()
        self.full_pair(unit, 0).start()

    def swap_cut(self, unit):
        for way in range(2):
            for core in range(2):
                self.transit_out(unit, way, core).start()
        self.cut_pair(unit).start()
        for way in range(2):
            for core in range(2):
                self.cut_out(unit, way, core).start()

    def full_2(self, unit):
        for way in range(2):
            self.full_out(unit, way).wait_recv()
            self.full_on(unit, way).start()
            self.full_pair(unit, 1 + way).start()

    def cut_2(self, unit):
        for way in range(2):
            for core in range(2):
                self.transit_out(unit, way, core).wait_recv()
                self.transit_on(unit, way, core).start()

    def full_3(self, unit):
        for way in range(2):
            self.full_on(unit, way).wait_recv()
        self.full_pair(unit, 3).start()


    @once
    def loads(self, unit):
        copies = []
        for j in range(8):
            rows = pl.ds(j * self.toks, self.toks)
            if j == 0:
                full, cut = self.full(unit), self.cut(unit, self.at[self.axis(unit, 0)], self.core)
            else:
                slot = self.slot(unit, j // 2, j % 2)
                full, cut = self.fx.at[unit, slot], self.sx.at[unit, slot]
            copies.append(pltpu.make_async_copy(full, self.fbuf.at[rows], self.load_sem.at[0, j]))
            copies.append(pltpu.make_async_copy(cut, self.sbuf.at[rows], self.load_sem.at[1, j]))
        return copies

    def load(self, unit):
        for j in range(4):
            self.full_pair(unit, j).wait_recv()
        self.cut_pair(unit).wait_recv()
        for way in range(2):
            for source in range(2):
                self.cut_out(unit, way, 0, source).wait_recv()
                self.transit_on(unit, way, 0, source).wait_recv()
        for copy in self.loads(unit):
            copy.start()

    def product(self, unit):
        for copy in self.loads(unit):
            copy.wait()
        if unit >= HELD:
            self.sent(unit - HELD)
        fbuf, sbuf, wp, edge = self.fbuf, self.sbuf, self.wp.at[unit % HELD], self.edge
        block = edge // 2

        def step(b, carry):
            rows = pl.ds(pl.multiple_of(b * block, block), block)
            if self.kind(unit) == OUT:
                for part in range(2):
                    cols = pl.ds(part * edge, edge)
                    wp[part, rows] = lax.dot_general(sbuf[:, rows], fbuf[:, cols], ROW_CONTRACT, preferred_element_type=F32)
            else:
                term = lax.dot_general(fbuf[:, rows], sbuf[:, :], ROW_CONTRACT, preferred_element_type=F32)
                wp[lax.div(b, 2), pl.ds(pl.multiple_of(lax.rem(b, 2) * block, block), block)] = term
            return carry

        lax.fori_loop(0, 2 if self.kind(unit) == OUT else 4, step, 0)
        for part in range(2):
            for way in range(2):
                self.rs(unit, part, 0, 0, way).start()


    def rs_axis(self, unit, part, phase):
        return self.axis(unit, 1 + (part + phase) % 2)

    @once
    def span(self, unit, part, phase, block, half=None):
        size = self.edge // RING
        base = 0
        if phase:
            base = self.at[self.rs_axis(unit, part, 0)] * size
            size //= RING
        row = base + self.ring(self.rs_axis(unit, part, phase), block) * size
        if half is not None:
            size //= 2
            row = row + half * size
        return pl.multiple_of(row, size), size

    @once
    def rs(self, unit, part, phase, step, way):
        if step == 0:
            row, size = self.span(unit, part, phase, 2, way)
            dst = self.near[phase]
        else:
            row, size = self.span(unit, part, phase, self.side(way))
            dst = self.far[phase]
        index = 21 + ((part * 2 + phase) * 2 + step) * 2 + way
        src = self.wp.at[unit % HELD, part, pl.ds(row, size)]
        return self.copy(unit, index, src, dst.at[unit, part, way], self.device(self.rs_axis(unit, part, phase), self.side(way)))

    def accumulate(self, unit, part, row, size, sources):
        chunk = min(16, size)

        def step(i, carry):
            at = pl.multiple_of(i * chunk, chunk)
            here = pl.ds(pl.multiple_of(row + at, chunk), chunk)
            total = self.wp[unit % HELD, part, here]
            for ref, way in sources:
                total = total + ref[unit, part, way, pl.ds(at, chunk)]
            self.wp[unit % HELD, part, here] = total
            return carry

        lax.fori_loop(0, size // chunk, step, 0)

    def reduce_near(self, unit, phase):
        for part in range(2):
            for way in range(2):
                self.rs(unit, part, phase, 0, way).wait_recv()
                row, size = self.span(unit, part, phase, self.side(way), way)
                self.accumulate(unit, part, row, size, [(self.near[phase], way)])
                self.rs(unit, part, phase, 1, way).start()

    def reduce_far(self, unit, phase):
        for part in range(2):
            for way in range(2):
                self.rs(unit, part, phase, 1, way).wait_recv()
            row, size = self.span(unit, part, phase, 0)
            self.accumulate(unit, part, row, size, [(self.far[phase], 0), (self.far[phase], 1)])
            for way in range(2):
                if phase == 0:
                    self.rs(unit, part, 1, 0, way).start()
                else:
                    self.ag(unit, part, 0, 0, way).start()
            if phase == 1:
                self.keep(unit, part).start()

    def reduce_2(self, unit):
        self.reduce_near(unit, 0)

    def reduce_3(self, unit):
        self.reduce_far(unit, 0)

    def reduce_4(self, unit):
        self.reduce_near(unit, 1)

    def reduce_5(self, unit):
        self.reduce_far(unit, 1)


    def result(self, unit, part, row, size, shift=None):
        layer, edge, piece = self.layer(unit), self.edge, self.piece
        if shift is None:
            first, count = self.core * RING, RING
        else:
            first, count = self.core * RING + self.ring(self.axis(unit, 0), shift), 1
        if self.kind(unit) == OUT:
            return self.r_out.at[layer, pl.ds(first, count), pl.ds(row, size), pl.ds(part * edge, edge)]
        cols = pl.ds(pl.multiple_of(first * piece, piece), count * piece)
        return self.r_in.at[layer, pl.ds(pl.multiple_of(part * edge + row, size), size), cols]

    def shard(self, unit, part):
        row, size = self.span(unit, part, 1, 0)
        return self.wp.at[unit % HELD, pl.ds(part, 1), pl.ds(row, size)] if self.kind(unit) == OUT else self.wp.at[unit % HELD, part, pl.ds(row, size)]

    @once
    def keep(self, unit, part):
        return pltpu.make_async_copy(
            self.shard(unit, part), self.result(unit, part, *self.span(unit, part, 1, 0), 0), self.own_sem.at[unit, part]
        )

    @once
    def ag(self, unit, part, phase, step, way):
        if phase == 0:
            axis = self.axis(unit, 0)
            row, size = self.span(unit, part, 1, 0)
            if step:
                size //= 2
                row = row + way * size
            dst = self.result(unit, part, pl.multiple_of(row, size), size, self.back(way) if step else 0)
            src = dst if step else self.shard(unit, part)
        else:
            axis = self.rs_axis(unit, part, 2 - phase)
            row, size = self.span(unit, part, 2 - phase, self.back(way), way) if step else self.span(unit, part, 2 - phase, 0)
            src = dst = self.result(unit, part, row, size)
        index = 37 + ((part * 3 + phase) * 2 + step) * 2 + way
        return self.copy(unit, index, src, dst, self.device(axis, self.side(way)))

    @once
    def pair(self, unit, part, j):
        block, half = ((0, None), (3, None), (1, None), (2, 0), (2, 1))[j]
        ref = self.result(unit, part, *self.span(unit, part, 0, block, half))
        return self.copy(unit, 61 + part * 5 + j, ref, ref, self.partner())

    def gather_on(self, unit, phase):
        for part in range(2):
            for way in range(2):
                self.ag(unit, part, phase, 0, way).wait_recv()
                self.ag(unit, part, phase, 1, way).start()
                if phase == 2:
                    self.pair(unit, part, 1 + way).start()

    def gather_next(self, unit, phase):
        for part in range(2):
            for way in range(2):
                self.ag(unit, part, phase - 1, 1, way).wait_recv()
            if phase == 1:
                self.keep(unit, part).wait()
            for way in range(2):
                self.ag(unit, part, phase, 0, way).start()
            if phase == 2:
                self.pair(unit, part, 0).start()

    def gather_1(self, unit):
        self.gather_on(unit, 0)

    def gather_2(self, unit):
        self.gather_next(unit, 1)

    def gather_3(self, unit):
        self.gather_on(unit, 1)

    def gather_4(self, unit):
        self.gather_next(unit, 2)

    def gather_5(self, unit):
        self.gather_on(unit, 2)

    def gather_6(self, unit):
        for part in range(2):
            for way in range(2):
                self.ag(unit, part, 2, 1, way).wait_recv()
                self.pair(unit, part, 3 + way).start()

    def sent(self, unit):
        for part in range(2):
            for way in range(2):
                for step in range(2):
                    for phase in range(2):
                        self.rs(unit, part, phase, step, way).wait_send()
                self.ag(unit, part, 0, 0, way).wait_send()

    def finish(self, unit):
        if unit + HELD >= 2 * self.layers:
            self.sent(unit)
        for part in range(2):
            for j in range(5):
                self.pair(unit, part, j).wait()
            for way in range(2):
                self.ag(unit, part, 0, 1, way).wait_send()
                for step in range(2):
                    for phase in (1, 2):
                        self.ag(unit, part, phase, step, way).wait_send()
        for way in range(2):
            self.full_out(unit, way).wait_send()
            self.full_on(unit, way).wait_send()
            for core in range(2):
                self.cut_out(unit, way, core).wait_send()
                self.transit_out(unit, way, core).wait_send()
                self.transit_on(unit, way, core).wait_send()
        for j in range(4):
            self.full_pair(unit, j).wait_send()
        self.cut_pair(unit).wait_send()

    def meet(self):
        barrier = pltpu.get_barrier_semaphore()
        others = [self.device(axis, shift, core) for axis in range(3) for shift in (1, 3) for core in range(2)]
        others.append(self.partner())
        for other in others:
            pl.semaphore_signal(barrier, inc=1, device_id=other, device_id_type=MESH)
        pl.semaphore_wait(barrier, len(others))

    def run(self):
        units = range(2 * self.layers)
        self.ahead(0, True)
        opening = self.move(self.tokens, self.cur)
        opening.start()
        self.meet()
        opening.wait()
        for code in ORDER:
            stage, unit = STAGES[code // 10], code % 10
            if unit < (self.layers if code < 20 else 2 * self.layers):
                getattr(self, stage)(unit)
        for unit in units:
            self.finish(unit)


def weight_grads(tokens, targets, w_in, w_out, inv_total):
    toks, dim = tokens.shape
    layers, _, hid = w_in.shape
    units, edge, piece, tile = 2 * layers, dim // 2, hid // 8, min(512, hid // 2)
    slots = min(4, hid // tile)
    assert edge == piece
    block, small = edge // RING, edge // RING**2

    def body(*refs):
        rest = refs[13:]
        near, far = (rest[3], rest[5]), (rest[4], rest[6])
        Reducer(refs[:4], refs[4:13], (*rest[:3], near, far, *rest[7:]), layers, toks, dim, hid, inv_total).run()

    anywhere = pl.BlockSpec(memory_space=pl.ANY)
    grad_in, grad_out, *_ = pl.pallas_call(
        body,
        in_specs=[anywhere] * 4,
        out_specs=[anywhere] * 9,
        out_shape=[
            jax.ShapeDtypeStruct((layers, dim, hid), F32),
            jax.ShapeDtypeStruct((layers, 8, piece, dim), F32),
            jax.ShapeDtypeStruct((units, 8, toks, dim), BF16),
            jax.ShapeDtypeStruct((units, 8, toks, piece), BF16),
            jax.ShapeDtypeStruct((units, 2, 2, toks // 2, piece), BF16),
            jax.ShapeDtypeStruct((layers, toks, dim), BF16),
            jax.ShapeDtypeStruct((layers, toks, hid), BF16),
            jax.ShapeDtypeStruct((layers, toks, hid), BF16),
            jax.ShapeDtypeStruct((layers, toks, dim), BF16),
        ],
        scratch_shapes=[
            pltpu.VMEM((8 * toks, dim), BF16),
            pltpu.VMEM((8 * toks, piece), BF16),
            pltpu.VMEM((min(HELD, units), 2, edge, edge), F32),
            pltpu.VMEM((units, 2, 2, block // 2, edge), F32),
            pltpu.VMEM((units, 2, 2, block, edge), F32),
            pltpu.VMEM((units, 2, 2, small // 2, edge), F32),
            pltpu.VMEM((units, 2, 2, small, edge), F32),
            pltpu.SemaphoreType.DMA((2, units, 71)),
            pltpu.SemaphoreType.DMA((2, 8)),
            pltpu.SemaphoreType.DMA((units, 2)),
            pltpu.VMEM((toks, dim), BF16),
            pltpu.VMEM((toks, dim), F32),
            pltpu.VMEM((layers, toks, hid), BF16),
            pltpu.VMEM((toks, hid), BF16),
            pltpu.VMEM((slots, dim, tile), BF16),
            pltpu.VMEM((slots, tile, dim), BF16),
            pltpu.SemaphoreType.DMA((slots, 2)),
            pltpu.SemaphoreType.DMA((hid // tile + 1,)),
        ],
        compiler_params=pltpu.CompilerParams(collective_id=1, has_side_effects=True, vmem_limit_bytes=63 << 20),
        cost_estimate=pl.CostEstimate(
            flops=12 * layers * toks * dim * hid, bytes_accessed=40 * layers * dim * hid, transcendentals=2 * layers * toks * hid
        ),
        name='weight_grads',
    )(tokens, targets, w_in, w_out)
    return grad_in, grad_out.reshape(layers, hid, dim)


def settle(arrays):
    blocks, ahead = 32, 4
    slots = 2 * ahead
    count = len(arrays)
    flat = [array.reshape(blocks, -1, array.shape[-1]) for array in arrays]

    def body(*refs):
        src, dst, held, sems = refs[:count], refs[count : 2 * count], refs[2 * count : 3 * count], refs[-1]

        def reads(i):
            slot = lax.rem(i, slots)
            return [pltpu.make_async_copy(src[k].at[i], held[k].at[slot], sems.at[0, k, slot]) for k in range(count)]

        def writes(i):
            slot = lax.rem(i, slots)
            return [pltpu.make_async_copy(held[k].at[slot], dst[k].at[i], sems.at[1, k, slot]) for k in range(count)]

        def step(i, carry):
            for read, write in zip(reads(i), writes(i)):
                read.wait()
                write.start()

            @pl.when((i >= ahead) & (i + ahead < blocks))
            def _():
                for write in writes(i - ahead):
                    write.wait()

            @pl.when(i + ahead < blocks)
            def _():
                for read in reads(i + ahead):
                    read.start()

            return carry

        def last(i, carry):
            for write in writes(i):
                write.wait()
            return carry

        for i in range(ahead):
            for read in reads(i):
                read.start()
        lax.fori_loop(0, blocks, step, 0)
        lax.fori_loop(blocks - slots, blocks, last, 0)

    anywhere = pl.BlockSpec(memory_space=pl.ANY)
    size = sum(array.size for array in arrays)
    out = pl.pallas_call(
        body,
        in_specs=[anywhere] * count,
        out_specs=[anywhere] * count,
        out_shape=[jax.ShapeDtypeStruct(x.shape, x.dtype) for x in flat],
        scratch_shapes=[pltpu.VMEM((slots, *x.shape[1:]), x.dtype) for x in flat] + [pltpu.SemaphoreType.DMA((2, count, slots))],
        compiler_params=pltpu.CompilerParams(vmem_limit_bytes=48 << 20),
        cost_estimate=pl.CostEstimate(flops=size, bytes_accessed=8 * size, transcendentals=0),
        name='settle',
    )(*flat)
    return [x.reshape(array.shape) for x, array in zip(out, arrays)]


def solution(mesh):
    def run(tokens, targets, w_in, w_out):
        inv_total = 1.0 / tokens.shape[0]

        def local_step(tok_local, tgt_local, w_first_all, w_second_all):
            return tuple(settle(weight_grads(tok_local, tgt_local, w_first_all, w_second_all, inv_total)))

        data_spec = P(DATA_AXES, None)
        mapped = jax.shard_map(local_step, mesh=mesh, in_specs=(data_spec, data_spec, P(), P()), out_specs=(P(), P()), check_vma=False)
        return mapped(tokens, targets, w_in, w_out)

    return run
```

```python
import functools

import jax
import jax.numpy as jnp
from jax import lax
from jax.experimental import pallas as pl
from jax.experimental.pallas import tpu as pltpu
from jax.sharding import PartitionSpec as P

DATA_AXES = ('dy', 'dx')
MESH = pl.DeviceIdType.MESH
RING = 4
ROW_CONTRACT = (((0,), (0,)), ((), ()))
COL_CONTRACT = (((1,), (1,)), ((), ()))
F32, BF16 = jnp.float32, jnp.bfloat16


OUT, IN = 0, 1
HELD = 5
STAGES = (
    'forward',
    'backward',
    'swap_full',
    'full_2',
    'full_3',
    'load',
    'product',
    'reduce_2',
    'reduce_3',
    'reduce_4',
    'reduce_5',
    'gather_1',
    'gather_2',
    'gather_3',
    'gather_4',
    'gather_5',
    'gather_6',
)
ORDER = (
    0, 1, 25, 23, 2, 21, 3, 20, 33, 13, 31, 22, 12, 24, 30, 11, 41, 40, 35, 43,
    50, 34, 27, 26, 32, 60, 42, 61, 52, 70, 37, 71, 62, 36, 47, 44, 80, 81, 45, 72,
    90, 91, 63, 54, 101, 100, 82, 111, 110, 92, 121, 64, 102, 131, 120, 73, 112, 46, 141, 65,
    56, 130, 74, 83, 66, 75, 122, 67, 93, 84, 85, 76, 95, 77, 105, 86, 103, 87, 94, 115,
    96, 132, 113, 97, 125, 106, 104, 142, 151, 135, 114, 116, 107, 140, 10, 145, 126, 117, 123, 124,
    150, 136, 127, 133, 146, 134, 152, 137, 155, 161, 156, 160, 143, 144, 166, 147, 153, 165, 162, 154,
    157, 163, 164, 167,
)
CROSSED = ((0, 1), (1, 0), (6, 0), (6, 1), (7, 0), (7, 1))


def once(method):
    @functools.wraps(method)
    def get(self, *args):
        key = method.__name__, args
        if key not in self.memo:
            self.memo[key] = method(self, *args)
        return self.memo[key]

    return get


class Reducer:
    def __init__(self, ins, outs, scratch, layers, toks, dim, hid, inv_total):
        self.tokens, self.targets, self.w_in, self.w_out = ins
        self.r_in, self.r_out, self.fx, self.h, self.g = outs
        self.fbuf, self.ubuf, self.sbuf, self.wp, self.near, self.far, self.sems, self.load_sem, self.own_sem, *local = scratch
        self.cur, self.acc, self.pre, self.w1, self.w2, self.w_sem, self.v1, self.v2, self.v_sem = local
        self.tile, self.slots = self.w1.shape[-1], self.w1.shape[0]
        self.tiles = hid // self.tile
        self.layers, self.toks, self.dim, self.hid = layers, toks, dim, hid
        self.memo = {}
        self.inv_total = inv_total
        self.piece, self.edge = hid // 8, dim // 2
        dx = lax.axis_index('dx')
        self.core = lax.rem(dx, 2)
        self.at = (lax.axis_index('dy'), lax.rem(lax.div(dx, 2), RING), lax.div(dx, 2 * RING))

    def kind(self, unit):
        return unit % 2

    def layer(self, unit):
        return self.layers - 1 - unit // 2

    def axis(self, unit, k):
        return (unit // 2 + k) % 3

    @once
    def ring(self, axis, shift):
        return lax.rem(self.at[axis] + shift, RING)

    @once
    def chip(self, axis, shift):
        x, y, z = (self.ring(i, shift) if i == axis else c for i, c in enumerate(self.at))
        return x, (z * RING + y) * 2

    @once
    def device(self, axis, shift, core=None):
        x, rest = self.chip(axis, shift)
        return x, rest + (self.core if core is None else core)

    @once
    def partner(self):
        x, rest = self.chip(None, 0)
        return x, rest + (1 - self.core)

    def copy(self, unit, index, src, dst, device, recv_index=None):
        recv = index if recv_index is None else recv_index
        return pltpu.make_async_remote_copy(
            src, dst, self.sems.at[0, unit, index], self.sems.at[1, unit, recv], device_id=device, device_id_type=MESH
        )


    def move(self, src, dst):
        copy = pltpu.make_async_copy(src, dst, self.own_sem.at[2 * self.layers, 0])
        copy.start()
        copy.wait()

    def fetch(self, layer, tile, first):
        part, slot = pl.ds(pl.multiple_of(tile * self.tile, self.tile), self.tile), lax.rem(tile, self.slots)
        copies = [pltpu.make_async_copy(self.w_out.at[layer, part], self.w2.at[slot], self.w_sem.at[slot, 1])]
        if first:
            copies.append(pltpu.make_async_copy(self.w_in.at[layer, :, part], self.w1.at[slot], self.w_sem.at[slot, 0]))
        return copies

    def ahead(self, layer, first):
        for tile in range(self.slots - 1):
            for copy in self.fetch(layer, tile, first):
                copy.start()

    def over_tiles(self, layer, first, following, work):
        tiles = self.tiles

        def step(tile, carry):
            for copy in self.fetch(layer, tile, first):
                copy.wait()
            later = tile + self.slots - 1

            @pl.when(later < tiles)
            def _():
                for copy in self.fetch(layer, later, first):
                    copy.start()

            if following is not None:

                @pl.when(later >= tiles)
                def _():
                    for copy in self.fetch(following[0], later - tiles, following[1]):
                        copy.start()

            work(lax.rem(tile, self.slots), pl.ds(pl.multiple_of(tile * self.tile, self.tile), self.tile))
            return carry

        lax.fori_loop(0, tiles, step, 0)

    def forward(self, layer):
        top = self.layers - 1

        def work(slot, part):
            pre_act = jnp.dot(self.cur[:, :], self.w1[slot], preferred_element_type=F32).astype(BF16)
            self.pre[layer, :, part] = pre_act
            post_act = jax.nn.gelu(pre_act.astype(F32)).astype(BF16)
            self.acc[:, :] += jnp.dot(post_act, self.w2[slot], preferred_element_type=F32)

        self.acc[:, :] = self.cur[:, :].astype(F32)
        following = (layer + 1, True) if layer < top else ((top, True) if top > 0 else None)
        self.over_tiles(layer, True, following, work)
        self.cur[:, :] = self.acc[:, :].astype(BF16)
        if layer == top:
            targets = self.fbuf.at[0, pl.ds(0, self.toks)]
            self.move(self.targets, targets)
            gap = self.cur[:, :].astype(F32) - targets[:, :].astype(F32)
            self.cur[:, :] = (gap * self.inv_total).astype(BF16)
        self.move(self.cur, self.h.at[layer + 1] if layer < top else self.g.at[top])

    def backward(self, layer):
        def work(slot, part):
            grad_post = lax.dot_general(self.cur[:, :], self.w2[slot], COL_CONTRACT, preferred_element_type=F32)
            pre_act = self.pre[layer, :, part].astype(F32)
            grad_pre = jax.vjp(jax.nn.gelu, pre_act)[1](grad_post)[0].astype(BF16)
            self.acc[:, :] += lax.dot_general(grad_pre, self.w1[slot], COL_CONTRACT, preferred_element_type=F32)

        if layer > 0:
            self.acc[:, :] = self.cur[:, :].astype(F32)
            self.over_tiles(layer, True, (layer - 1, True) if layer > 1 else None, work)
            self.cur[:, :] = self.acc[:, :].astype(BF16)
            self.move(self.cur, self.g.at[layer - 1])


    def full(self, unit):
        layer = self.layer(unit)
        if self.kind(unit) == IN and layer == 0:
            return self.tokens
        return (self.g, self.h)[self.kind(unit)].at[layer]

    def side(self, way):
        return 1 + 2 * way

    def back(self, way):
        return RING - self.side(way)

    def half(self, way):
        return way * (self.toks // 2), self.toks // 2

    @once
    def slot(self, unit, shift, other=0):
        return self.ring(self.axis(unit, 0), shift) * 2 + (1 - self.core if other else self.core)

    @once
    def full_out(self, unit, way):
        ref = self.fx.at[unit, self.slot(unit, 0)]
        return self.copy(unit, way, self.full(unit), ref, self.device(self.axis(unit, 0), self.side(way)))

    @once
    def full_on(self, unit, way):
        ref = self.fx.at[unit, self.slot(unit, self.back(way)), pl.ds(*self.half(way))]
        return self.copy(unit, 2 + way, ref, ref, self.device(self.axis(unit, 0), self.side(way)))

    @once
    def full_pair(self, unit, j):
        ref = self.fx.at[unit, self.slot(unit, (0, 3, 1, 2)[j])]
        return self.copy(unit, 4 + j, self.full(unit) if j == 0 else ref, ref, self.partner())

    def swap_full(self, unit):
        for way in range(2):
            self.full_out(unit, way).start()
        self.full_pair(unit, 0).start()

    def full_2(self, unit):
        for way in range(2):
            self.full_out(unit, way).wait_recv()
            self.full_on(unit, way).start()
            self.full_pair(unit, 1 + way).start()

    def full_3(self, unit):
        for way in range(2):
            self.full_on(unit, way).wait_recv()
        self.full_pair(unit, 3).start()


    @once
    def loads(self, unit):
        copies = []
        for k, one in enumerate((unit, unit + 1)):
            for j in range(8):
                src = self.fx.at[one, self.slot(one, j // 2, j % 2)] if j else self.full(one)
                copies.append(pltpu.make_async_copy(src, self.fbuf.at[k, pl.ds(j * self.toks, self.toks)], self.load_sem.at[k, j]))
        layer = self.layer(unit)
        place = self.core * RING + self.at[self.axis(unit, 0)]
        share = pl.ds(pl.multiple_of(place * self.piece, self.piece), self.piece)
        copies.append(pltpu.make_async_copy(self.w_in.at[layer, :, share], self.v1, self.v_sem.at[0]))
        copies.append(pltpu.make_async_copy(self.w_out.at[layer, share], self.v2, self.v_sem.at[1]))
        return copies

    def load(self, unit):
        for one in (unit, unit + 1):
            for j in range(4):
                self.full_pair(one, j).wait_recv()
        for copy in self.loads(unit):
            copy.start()

    def over_rows(self, work):
        def step(j, carry):
            work(pl.ds(pl.multiple_of(j * self.toks, self.toks), self.toks))
            return carry

        lax.fori_loop(0, 8, step, 0)

    def again(self, rows):
        pre_act = jnp.dot(self.fbuf[1, rows], self.v1[:, :], preferred_element_type=F32).astype(BF16)
        self.ubuf[rows, :] = pre_act
        self.sbuf[rows, :] = jax.nn.gelu(pre_act.astype(F32)).astype(BF16)

    def again_back(self, rows):
        grad_post = lax.dot_general(self.fbuf[0, rows], self.v2[:, :], COL_CONTRACT, preferred_element_type=F32)
        pre_act = self.ubuf[rows, :].astype(F32)
        self.sbuf[rows, :] = jax.vjp(jax.nn.gelu, pre_act)[1](grad_post)[0].astype(BF16)

    def product(self, unit):
        if unit >= HELD:
            self.sent(unit - HELD)
        if self.kind(unit) == OUT:
            for copy in self.loads(unit):
                copy.wait()
        self.over_rows(self.again if self.kind(unit) == OUT else self.again_back)
        sbuf, wp, edge = self.sbuf, self.wp.at[unit % HELD], self.edge
        block = edge // 2

        def step(b, carry):
            rows = pl.ds(pl.multiple_of(b * block, block), block)
            if self.kind(unit) == OUT:
                for part in range(2):
                    grads = self.fbuf[0, :, pl.ds(part * edge, edge)]
                    wp[part, rows] = lax.dot_general(sbuf[:, rows], grads, ROW_CONTRACT, preferred_element_type=F32)
            else:
                term = lax.dot_general(self.fbuf[1, :, rows], sbuf[:, :], ROW_CONTRACT, preferred_element_type=F32)
                wp[lax.div(b, 2), pl.ds(pl.multiple_of(lax.rem(b, 2) * block, block), block)] = term
            return carry

        lax.fori_loop(0, 2 if self.kind(unit) == OUT else 4, step, 0)
        for part in range(2):
            for way in range(2):
                self.rs(unit, part, 0, 0, way).start()


    def rs_axis(self, unit, part, phase):
        return self.axis(unit, 1 + (part + phase) % 2)

    @once
    def span(self, unit, part, phase, block, half=None):
        size = self.edge // RING
        base = 0
        if phase:
            base = self.at[self.rs_axis(unit, part, 0)] * size
            size //= RING
        row = base + self.ring(self.rs_axis(unit, part, phase), block) * size
        if half is not None:
            size //= 2
            row = row + half * size
        return pl.multiple_of(row, size), size

    @once
    def rs(self, unit, part, phase, step, way):
        if step == 0:
            row, size = self.span(unit, part, phase, 2, way)
            dst = self.near[phase]
        else:
            row, size = self.span(unit, part, phase, self.side(way))
            dst = self.far[phase]
        index = 8 + ((part * 2 + phase) * 2 + step) * 2 + way
        src = self.wp.at[unit % HELD, part, pl.ds(row, size)]
        return self.copy(unit, index, src, dst.at[unit, part, way], self.device(self.rs_axis(unit, part, phase), self.side(way)))

    def accumulate(self, unit, part, row, size, sources):
        chunk = min(16, size)

        def step(i, carry):
            at = pl.multiple_of(i * chunk, chunk)
            here = pl.ds(pl.multiple_of(row + at, chunk), chunk)
            total = self.wp[unit % HELD, part, here]
            for ref, way in sources:
                total = total + ref[unit, part, way, pl.ds(at, chunk)]
            self.wp[unit % HELD, part, here] = total
            return carry

        lax.fori_loop(0, size // chunk, step, 0)

    def reduce_near(self, unit, phase):
        for part in range(2):
            for way in range(2):
                self.rs(unit, part, phase, 0, way).wait_recv()
                row, size = self.span(unit, part, phase, self.side(way), way)
                self.accumulate(unit, part, row, size, [(self.near[phase], way)])
                self.rs(unit, part, phase, 1, way).start()

    def reduce_far(self, unit, phase):
        for part in range(2):
            for way in range(2):
                self.rs(unit, part, phase, 1, way).wait_recv()
            row, size = self.span(unit, part, phase, 0)
            self.accumulate(unit, part, row, size, [(self.far[phase], 0), (self.far[phase], 1)])
            for way in range(2):
                if phase == 0:
                    self.rs(unit, part, 1, 0, way).start()
                else:
                    self.ag(unit, part, 0, 0, way).start()
            if phase == 1:
                self.keep(unit, part).start()

    def reduce_2(self, unit):
        self.reduce_near(unit, 0)

    def reduce_3(self, unit):
        self.reduce_far(unit, 0)

    def reduce_4(self, unit):
        self.reduce_near(unit, 1)

    def reduce_5(self, unit):
        self.reduce_far(unit, 1)


    def result(self, unit, part, row, size, shift=None):
        layer, edge, piece = self.layer(unit), self.edge, self.piece
        if shift is None:
            first, count = self.core * RING, RING
        else:
            first, count = self.core * RING + self.ring(self.axis(unit, 0), shift), 1
        if self.kind(unit) == OUT:
            return self.r_out.at[layer, pl.ds(first, count), pl.ds(row, size), pl.ds(part * edge, edge)]
        cols = pl.ds(pl.multiple_of(first * piece, piece), count * piece)
        return self.r_in.at[layer, pl.ds(pl.multiple_of(part * edge + row, size), size), cols]

    def shard(self, unit, part):
        row, size = self.span(unit, part, 1, 0)
        return self.wp.at[unit % HELD, pl.ds(part, 1), pl.ds(row, size)] if self.kind(unit) == OUT else self.wp.at[unit % HELD, part, pl.ds(row, size)]

    @once
    def keep(self, unit, part):
        return pltpu.make_async_copy(
            self.shard(unit, part), self.result(unit, part, *self.span(unit, part, 1, 0), 0), self.own_sem.at[unit, part]
        )

    @once
    def ag(self, unit, part, phase, step, way):
        axis, block, half = self.rs_axis(unit, part, 0), 0, None
        if step:
            block, half = self.back(way), way
        if phase == 2:
            src = dst = self.result(unit, part, *self.span(unit, part, 0, block, half))
        elif (phase == 0) == ((unit, part) in CROSSED):
            axis = self.rs_axis(unit, part, 1)
            dst = self.result(unit, part, *self.span(unit, part, 1, block, half), 0 if phase == 0 else None)
            src = dst
        else:
            axis = self.axis(unit, 0)
            dst = self.result(unit, part, *self.span(unit, part, 1 - phase, 0, half), block)
            src = dst
        if phase == 0 and step == 0:
            src = self.shard(unit, part)
        index = 24 + ((part * 3 + phase) * 2 + step) * 2 + way
        return self.copy(unit, index, src, dst, self.device(axis, self.side(way)))

    @once
    def pair(self, unit, part, j):
        block, half = ((0, None), (3, None), (1, None), (2, 0), (2, 1))[j]
        ref = self.result(unit, part, *self.span(unit, part, 0, block, half))
        return self.copy(unit, 48 + part * 5 + j, ref, ref, self.partner())

    def gather_on(self, unit, phase):
        for part in range(2):
            for way in range(2):
                self.ag(unit, part, phase, 0, way).wait_recv()
                self.ag(unit, part, phase, 1, way).start()
                if phase == 2:
                    self.pair(unit, part, 1 + way).start()

    def gather_next(self, unit, phase):
        for part in range(2):
            for way in range(2):
                self.ag(unit, part, phase - 1, 1, way).wait_recv()
            if phase == 1:
                self.keep(unit, part).wait()
            for way in range(2):
                self.ag(unit, part, phase, 0, way).start()
            if phase == 2:
                self.pair(unit, part, 0).start()

    def gather_1(self, unit):
        self.gather_on(unit, 0)

    def gather_2(self, unit):
        self.gather_next(unit, 1)

    def gather_3(self, unit):
        self.gather_on(unit, 1)

    def gather_4(self, unit):
        self.gather_next(unit, 2)

    def gather_5(self, unit):
        self.gather_on(unit, 2)

    def gather_6(self, unit):
        for part in range(2):
            for way in range(2):
                self.ag(unit, part, 2, 1, way).wait_recv()
                self.pair(unit, part, 3 + way).start()

    def sent(self, unit):
        for part in range(2):
            for way in range(2):
                for step in range(2):
                    for phase in range(2):
                        self.rs(unit, part, phase, step, way).wait_send()
                self.ag(unit, part, 0, 0, way).wait_send()

    def finish(self, unit):
        if unit + HELD >= 2 * self.layers:
            self.sent(unit)
        for part in range(2):
            for j in range(5):
                self.pair(unit, part, j).wait()
            for way in range(2):
                self.ag(unit, part, 0, 1, way).wait_send()
                for step in range(2):
                    for phase in (1, 2):
                        self.ag(unit, part, phase, step, way).wait_send()
        for way in range(2):
            self.full_out(unit, way).wait_send()
            self.full_on(unit, way).wait_send()
        for j in range(4):
            self.full_pair(unit, j).wait_send()

    def meet(self):
        barrier = pltpu.get_barrier_semaphore()
        others = [self.device(axis, shift) for axis in range(3) for shift in (1, 3)] + [self.partner()]
        for other in others:
            pl.semaphore_signal(barrier, inc=1, device_id=other, device_id_type=MESH)
        pl.semaphore_wait(barrier, len(others))

    def run(self):
        units = range(2 * self.layers)
        self.ahead(0, True)
        self.move(self.tokens, self.cur)
        self.meet()
        for code in ORDER:
            stage, unit = STAGES[code // 10], code % 10
            if unit < (self.layers if code < 20 else 2 * self.layers):
                getattr(self, stage)(unit)
        for unit in units:
            self.finish(unit)


def weight_grads(tokens, targets, w_in, w_out, inv_total):
    toks, dim = tokens.shape
    layers, _, hid = w_in.shape
    units, edge, piece, tile = 2 * layers, dim // 2, hid // 8, min(512, hid // 2)
    slots = min(4, hid // tile)
    assert edge == piece
    block, small = edge // RING, edge // RING**2

    def body(*refs):
        rest = refs[9:]
        near, far = (rest[4], rest[6]), (rest[5], rest[7])
        Reducer(refs[:4], refs[4:9], (*rest[:4], near, far, *rest[8:]), layers, toks, dim, hid, inv_total).run()

    anywhere = pl.BlockSpec(memory_space=pl.ANY)
    grad_in, grad_out, *_ = pl.pallas_call(
        body,
        in_specs=[anywhere] * 4,
        out_specs=[anywhere] * 5,
        out_shape=[
            jax.ShapeDtypeStruct((layers, dim, hid), F32),
            jax.ShapeDtypeStruct((layers, 8, piece, dim), F32),
            jax.ShapeDtypeStruct((units, 8, toks, dim), BF16),
            jax.ShapeDtypeStruct((layers, toks, dim), BF16),
            jax.ShapeDtypeStruct((layers, toks, dim), BF16),
        ],
        scratch_shapes=[
            pltpu.VMEM((2, 8 * toks, dim), BF16),
            pltpu.VMEM((8 * toks, piece), BF16),
            pltpu.VMEM((8 * toks, piece), BF16),
            pltpu.VMEM((min(HELD, units), 2, edge, edge), F32),
            pltpu.VMEM((units, 2, 2, block // 2, edge), F32),
            pltpu.VMEM((units, 2, 2, block, edge), F32),
            pltpu.VMEM((units, 2, 2, small // 2, edge), F32),
            pltpu.VMEM((units, 2, 2, small, edge), F32),
            pltpu.SemaphoreType.DMA((2, units, 58)),
            pltpu.SemaphoreType.DMA((2, 8)),
            pltpu.SemaphoreType.DMA((units + 1, 2)),
            pltpu.VMEM((toks, dim), BF16),
            pltpu.VMEM((toks, dim), F32),
            pltpu.VMEM((layers, toks, hid), BF16),
            pltpu.VMEM((slots, dim, tile), BF16),
            pltpu.VMEM((slots, tile, dim), BF16),
            pltpu.SemaphoreType.DMA((slots, 2)),
            pltpu.VMEM((dim, piece), BF16),
            pltpu.VMEM((piece, dim), BF16),
            pltpu.SemaphoreType.DMA((2,)),
        ],
        compiler_params=pltpu.CompilerParams(collective_id=1, has_side_effects=True, vmem_limit_bytes=63 << 20),
        cost_estimate=pl.CostEstimate(
            flops=16 * layers * toks * dim * hid, bytes_accessed=40 * layers * dim * hid, transcendentals=2 * layers * toks * hid
        ),
        name='weight_grads',
    )(tokens, targets, w_in, w_out)
    return grad_in, grad_out.reshape(layers, hid, dim)


def settle(arrays):
    blocks, ahead = 32, 4
    slots = 2 * ahead
    count = len(arrays)
    flat = [array.reshape(blocks, -1, array.shape[-1]) for array in arrays]

    def body(*refs):
        src, dst, held, sems = refs[:count], refs[count : 2 * count], refs[2 * count : 3 * count], refs[-1]

        def reads(i):
            slot = lax.rem(i, slots)
            return [pltpu.make_async_copy(src[k].at[i], held[k].at[slot], sems.at[0, k, slot]) for k in range(count)]

        def writes(i):
            slot = lax.rem(i, slots)
            return [pltpu.make_async_copy(held[k].at[slot], dst[k].at[i], sems.at[1, k, slot]) for k in range(count)]

        def step(i, carry):
            for read, write in zip(reads(i), writes(i)):
                read.wait()
                write.start()

            @pl.when((i >= ahead) & (i + ahead < blocks))
            def _():
                for write in writes(i - ahead):
                    write.wait()

            @pl.when(i + ahead < blocks)
            def _():
                for read in reads(i + ahead):
                    read.start()

            return carry

        def last(i, carry):
            for write in writes(i):
                write.wait()
            return carry

        for i in range(ahead):
            for read in reads(i):
                read.start()
        lax.fori_loop(0, blocks, step, 0)
        lax.fori_loop(blocks - slots, blocks, last, 0)

    anywhere = pl.BlockSpec(memory_space=pl.ANY)
    size = sum(array.size for array in arrays)
    out = pl.pallas_call(
        body,
        in_specs=[anywhere] * count,
        out_specs=[anywhere] * count,
        out_shape=[jax.ShapeDtypeStruct(x.shape, x.dtype) for x in flat],
        scratch_shapes=[pltpu.VMEM((slots, *x.shape[1:]), x.dtype) for x in flat] + [pltpu.SemaphoreType.DMA((2, count, slots))],
        compiler_params=pltpu.CompilerParams(vmem_limit_bytes=48 << 20),
        cost_estimate=pl.CostEstimate(flops=size, bytes_accessed=8 * size, transcendentals=0),
        name='settle',
    )(*flat)
    return [x.reshape(array.shape) for x, array in zip(out, arrays)]


def solution(mesh):
    def run(tokens, targets, w_in, w_out):
        inv_total = 1.0 / tokens.shape[0]

        def local_step(tok_local, tgt_local, w_first_all, w_second_all):
            return tuple(settle(weight_grads(tok_local, tgt_local, w_first_all, w_second_all, inv_total)))

        data_spec = P(DATA_AXES, None)
        mapped = jax.shard_map(local_step, mesh=mesh, in_specs=(data_spec, data_spec, P(), P()), out_specs=(P(), P()), check_vma=False)
        return mapped(tokens, targets, w_in, w_out)

    return run
```

```python
import functools

import jax
import jax.numpy as jnp
from jax import lax
from jax.experimental import pallas as pl
from jax.experimental.pallas import tpu as pltpu
from jax.sharding import PartitionSpec as P

DATA_AXES = ('dy', 'dx')
MESH = pl.DeviceIdType.MESH
RING = 4
ROW_CONTRACT = (((0,), (0,)), ((), ()))
COL_CONTRACT = (((1,), (1,)), ((), ()))
F32, BF16 = jnp.float32, jnp.bfloat16


OUT, IN = 0, 1
HELD = 5
STAGES = (
    'forward',
    'backward',
    'swap_full',
    'full_2',
    'full_3',
    'load',
    'again',
    'product',
    'reduce_2',
    'reduce_3',
    'reduce_4',
    'reduce_5',
    'gather_1',
    'gather_2',
    'gather_3',
    'gather_4',
    'gather_5',
    'gather_6',
)
ORDER = (
    0, 1, 2, 21, 25, 23, 3, 31, 35, 20, 13, 22, 33, 41, 12, 24, 51, 32, 30, 27,
    11, 40, 61, 50, 26, 45, 43, 42, 34, 70, 71, 53, 36, 44, 37, 80, 52, 63, 81, 72,
    90, 73, 55, 91, 100, 82, 54, 65, 110, 74, 92, 47, 120, 46, 101, 84, 102, 130, 75, 56,
    57, 112, 111, 94, 10, 140, 83, 85, 121, 104, 122, 150, 93, 131, 114, 67, 76, 132, 77, 95,
    103, 86, 87, 96, 141, 113, 124, 97, 106, 142, 105, 107, 116, 134, 115, 117, 126, 160, 152, 127,
    125, 123, 144, 151, 136, 146, 137, 135, 133, 156, 145, 147, 161, 143, 162, 155, 171, 166, 170, 157,
    154, 153, 176, 165, 167, 172, 164, 163, 175, 177, 173, 174,
)
CROSSED = ((0, 1), (1, 0), (6, 0), (6, 1), (7, 0), (7, 1))


def once(method):
    @functools.wraps(method)
    def get(self, *args):
        key = method.__name__, args
        if key not in self.memo:
            self.memo[key] = method(self, *args)
        return self.memo[key]

    return get


class Reducer:
    def __init__(self, ins, outs, scratch, layers, toks, dim, hid, inv_total):
        self.tokens, self.targets, self.w_in, self.w_out = ins
        self.r_in, self.r_out, self.fx, self.h, self.g = outs
        self.fbuf, self.ubuf, self.sbuf, self.wp, self.near, self.far, self.sems, self.load_sem, self.own_sem, *local = scratch
        self.cur, self.acc, self.pre, self.w1, self.w2, self.w_sem, self.v1, self.v2, self.v_sem = local
        self.tile, self.slots = self.w1.shape[-1], self.w1.shape[0]
        self.tiles = hid // self.tile
        self.layers, self.toks, self.dim, self.hid = layers, toks, dim, hid
        self.memo = {}
        self.unsaved = None
        self.inv_total = inv_total
        self.piece, self.edge = hid // 8, dim // 2
        dx = lax.axis_index('dx')
        self.core = lax.rem(dx, 2)
        self.at = (lax.axis_index('dy'), lax.rem(lax.div(dx, 2), RING), lax.div(dx, 2 * RING))

    def kind(self, unit):
        return unit % 2

    def layer(self, unit):
        return self.layers - 1 - unit // 2

    def axis(self, unit, k):
        return (unit // 2 + k) % 3

    @once
    def ring(self, axis, shift):
        return lax.rem(self.at[axis] + shift, RING)

    @once
    def chip(self, axis, shift):
        x, y, z = (self.ring(i, shift) if i == axis else c for i, c in enumerate(self.at))
        return x, (z * RING + y) * 2

    @once
    def device(self, axis, shift, core=None):
        x, rest = self.chip(axis, shift)
        return x, rest + (self.core if core is None else core)

    @once
    def partner(self):
        x, rest = self.chip(None, 0)
        return x, rest + (1 - self.core)

    def copy(self, unit, index, src, dst, device, recv_index=None):
        recv = index if recv_index is None else recv_index
        return pltpu.make_async_remote_copy(
            src, dst, self.sems.at[0, unit, index], self.sems.at[1, unit, recv], device_id=device, device_id_type=MESH
        )


    def move(self, src, dst):
        copy = pltpu.make_async_copy(src, dst, self.own_sem.at[2 * self.layers, 0])
        copy.start()
        copy.wait()

    def save(self, place):
        self.unsaved = pltpu.make_async_copy(self.cur, place, self.own_sem.at[2 * self.layers, 1])
        self.unsaved.start()

    def saved(self):
        if self.unsaved is not None:
            self.unsaved.wait()
            self.unsaved = None

    def fetch(self, layer, tile, first):
        part, slot = pl.ds(pl.multiple_of(tile * self.tile, self.tile), self.tile), lax.rem(tile, self.slots)
        copies = [pltpu.make_async_copy(self.w_out.at[layer, part], self.w2.at[slot], self.w_sem.at[slot, 1])]
        if first:
            copies.append(pltpu.make_async_copy(self.w_in.at[layer, :, part], self.w1.at[slot], self.w_sem.at[slot, 0]))
        return copies

    def ahead(self, layer, first):
        for tile in range(self.slots - 1):
            for copy in self.fetch(layer, tile, first):
                copy.start()

    def over_tiles(self, layer, first, following, work):
        tiles = self.tiles

        def step(tile, carry):
            for copy in self.fetch(layer, tile, first):
                copy.wait()
            later = tile + self.slots - 1

            @pl.when(later < tiles)
            def _():
                for copy in self.fetch(layer, later, first):
                    copy.start()

            if following is not None:

                @pl.when(later >= tiles)
                def _():
                    for copy in self.fetch(following[0], later - tiles, following[1]):
                        copy.start()

            work(lax.rem(tile, self.slots), pl.ds(pl.multiple_of(tile * self.tile, self.tile), self.tile))
            return carry

        lax.fori_loop(0, tiles, step, 0)

    def forward(self, layer):
        top = self.layers - 1

        def work(slot, part):
            pre_act = jnp.dot(self.cur[:, :], self.w1[slot], preferred_element_type=F32).astype(BF16)
            self.pre[layer, :, part] = pre_act
            post_act = jax.nn.gelu(pre_act.astype(F32)).astype(BF16)
            self.acc[:, :] += jnp.dot(post_act, self.w2[slot], preferred_element_type=F32)

        self.acc[:, :] = self.cur[:, :].astype(F32)
        following = (layer + 1, True) if layer < top else ((top, True) if top > 0 else None)
        self.over_tiles(layer, True, following, work)
        self.saved()
        self.cur[:, :] = self.acc[:, :].astype(BF16)
        if layer == top:
            targets = self.fbuf.at[0, pl.ds(0, self.toks)]
            self.move(self.targets, targets)
            gap = self.cur[:, :].astype(F32) - targets[:, :].astype(F32)
            self.cur[:, :] = (gap * self.inv_total).astype(BF16)
        self.save(self.h.at[layer + 1] if layer < top else self.g.at[top])

    def backward(self, layer):
        def work(slot, part):
            grad_post = lax.dot_general(self.cur[:, :], self.w2[slot], COL_CONTRACT, preferred_element_type=F32)
            pre_act = self.pre[layer, :, part].astype(F32)
            grad_pre = jax.vjp(jax.nn.gelu, pre_act)[1](grad_post)[0].astype(BF16)
            self.acc[:, :] += lax.dot_general(grad_pre, self.w1[slot], COL_CONTRACT, preferred_element_type=F32)

        if layer > 0:
            self.acc[:, :] = self.cur[:, :].astype(F32)
            self.over_tiles(layer, True, (layer - 1, True) if layer > 1 else None, work)
            self.saved()
            self.cur[:, :] = self.acc[:, :].astype(BF16)
            self.save(self.g.at[layer - 1])


    def full(self, unit):
        layer = self.layer(unit)
        if self.kind(unit) == IN and layer == 0:
            return self.tokens
        return (self.g, self.h)[self.kind(unit)].at[layer]

    def side(self, way):
        return 1 + 2 * way

    def back(self, way):
        return RING - self.side(way)

    def half(self, way):
        return way * (self.toks // 2), self.toks // 2

    @once
    def slot(self, unit, shift, other=0):
        return self.ring(self.axis(unit, 0), shift) * 2 + (1 - self.core if other else self.core)

    @once
    def full_out(self, unit, way, later):
        rows = pl.ds(*self.half(1 - way if later else way))
        dst = self.fx.at[unit, self.slot(unit, 0), rows]
        return self.copy(unit, 2 * later + way, self.full(unit).at[rows], dst, self.device(self.axis(unit, 0), self.side(way)))

    @once
    def full_on(self, unit, way):
        ref = self.fx.at[unit, self.slot(unit, self.back(way)), pl.ds(*self.half(way))]
        return self.copy(unit, 4 + way, ref, ref, self.device(self.axis(unit, 0), self.side(way)))

    @once
    def full_pair(self, unit, j):
        ref = self.fx.at[unit, self.slot(unit, (0, 3, 1, 2)[j])]
        return self.copy(unit, 6 + j, self.full(unit) if j == 0 else ref, ref, self.partner())

    def swap_full(self, unit):
        self.saved()
        for later in range(2):
            for way in range(2):
                self.full_out(unit, way, later).start()
        self.full_pair(unit, 0).start()

    def full_2(self, unit):
        for way in range(2):
            self.full_out(unit, way, 0).wait_recv()
            self.full_on(unit, way).start()

    def full_3(self, unit):
        for way in range(2):
            self.full_out(unit, way, 1).wait_recv()
            self.full_pair(unit, 1 + way).start()
        for way in range(2):
            self.full_on(unit, way).wait_recv()
        self.full_pair(unit, 3).start()


    @once
    def loads(self, unit):
        kind, layer, copies = self.kind(unit), self.layer(unit), []
        for j in range(8):
            src = self.fx.at[unit, self.slot(unit, j // 2, j % 2)] if j else self.full(unit)
            copies.append(pltpu.make_async_copy(src, self.fbuf.at[kind, pl.ds(j * self.toks, self.toks)], self.load_sem.at[kind, j]))
        if kind == IN:
            place = self.core * RING + self.at[self.axis(unit, 0)]
            share = pl.ds(pl.multiple_of(place * self.piece, self.piece), self.piece)
            copies.append(pltpu.make_async_copy(self.w_in.at[layer, :, share], self.v1, self.v_sem.at[0]))
            copies.append(pltpu.make_async_copy(self.w_out.at[layer, share], self.v2, self.v_sem.at[1]))
        return copies

    def load(self, unit):
        for j in range(4):
            self.full_pair(unit, j).wait_recv()
        for copy in self.loads(unit):
            copy.start()

    def again(self, unit):
        for copy in self.loads(unit):
            copy.wait()
        self.over_rows(self.again_rows)

    def over_rows(self, work):
        def step(j, carry):
            work(pl.ds(pl.multiple_of(j * self.toks, self.toks), self.toks))
            return carry

        lax.fori_loop(0, 8, step, 0)

    def again_rows(self, rows):
        pre_act = jnp.dot(self.fbuf[1, rows], self.v1[:, :], preferred_element_type=F32).astype(BF16)
        self.ubuf[rows, :] = pre_act
        self.sbuf[rows, :] = jax.nn.gelu(pre_act.astype(F32)).astype(BF16)

    def again_back(self, rows):
        grad_post = lax.dot_general(self.fbuf[0, rows], self.v2[:, :], COL_CONTRACT, preferred_element_type=F32)
        pre_act = self.ubuf[rows, :].astype(F32)
        self.sbuf[rows, :] = jax.vjp(jax.nn.gelu, pre_act)[1](grad_post)[0].astype(BF16)

    def product(self, unit):
        if unit >= HELD:
            self.sent(unit - HELD)
        if self.kind(unit) == OUT:
            for copy in self.loads(unit):
                copy.wait()
        else:
            self.over_rows(self.again_back)
        sbuf, wp, edge = self.sbuf, self.wp.at[unit % HELD], self.edge
        block = edge // 2

        def step(b, carry):
            rows = pl.ds(pl.multiple_of(b * block, block), block)
            if self.kind(unit) == OUT:
                for part in range(2):
                    grads = self.fbuf[0, :, pl.ds(part * edge, edge)]
                    wp[part, rows] = lax.dot_general(sbuf[:, rows], grads, ROW_CONTRACT, preferred_element_type=F32)
            else:
                term = lax.dot_general(self.fbuf[1, :, rows], sbuf[:, :], ROW_CONTRACT, preferred_element_type=F32)
                wp[lax.div(b, 2), pl.ds(pl.multiple_of(lax.rem(b, 2) * block, block), block)] = term
            return carry

        lax.fori_loop(0, 2 if self.kind(unit) == OUT else 4, step, 0)
        for part in range(2):
            for way in range(2):
                self.rs(unit, part, 0, 0, way).start()


    def rs_axis(self, unit, part, phase):
        return self.axis(unit, 1 + (part + phase) % 2)

    @once
    def span(self, unit, part, phase, block, half=None):
        size = self.edge // RING
        base = 0
        if phase:
            base = self.at[self.rs_axis(unit, part, 0)] * size
            size //= RING
        row = base + self.ring(self.rs_axis(unit, part, phase), block) * size
        if half is not None:
            size //= 2
            row = row + half * size
        return pl.multiple_of(row, size), size

    @once
    def rs(self, unit, part, phase, step, way):
        if step == 0:
            row, size = self.span(unit, part, phase, 2, way)
            dst = self.near[phase]
        else:
            row, size = self.span(unit, part, phase, self.side(way))
            dst = self.far[phase]
        index = 10 + ((part * 2 + phase) * 2 + step) * 2 + way
        src = self.wp.at[unit % HELD, part, pl.ds(row, size)]
        return self.copy(unit, index, src, dst.at[unit, part, way], self.device(self.rs_axis(unit, part, phase), self.side(way)))

    def accumulate(self, unit, part, row, size, sources):
        chunk = min(16, size)

        def step(i, carry):
            at = pl.multiple_of(i * chunk, chunk)
            here = pl.ds(pl.multiple_of(row + at, chunk), chunk)
            total = self.wp[unit % HELD, part, here]
            for ref, way in sources:
                total = total + ref[unit, part, way, pl.ds(at, chunk)]
            self.wp[unit % HELD, part, here] = total
            return carry

        lax.fori_loop(0, size // chunk, step, 0)

    def reduce_near(self, unit, phase):
        for part in range(2):
            for way in range(2):
                self.rs(unit, part, phase, 0, way).wait_recv()
                row, size = self.span(unit, part, phase, self.side(way), way)
                self.accumulate(unit, part, row, size, [(self.near[phase], way)])
                self.rs(unit, part, phase, 1, way).start()

    def reduce_far(self, unit, phase):
        for part in range(2):
            for way in range(2):
                self.rs(unit, part, phase, 1, way).wait_recv()
            row, size = self.span(unit, part, phase, 0)
            self.accumulate(unit, part, row, size, [(self.far[phase], 0), (self.far[phase], 1)])
            for way in range(2):
                if phase == 0:
                    self.rs(unit, part, 1, 0, way).start()
                else:
                    self.ag(unit, part, 0, 0, way).start()
            if phase == 1:
                self.keep(unit, part).start()

    def reduce_2(self, unit):
        self.reduce_near(unit, 0)

    def reduce_3(self, unit):
        self.reduce_far(unit, 0)

    def reduce_4(self, unit):
        self.reduce_near(unit, 1)

    def reduce_5(self, unit):
        self.reduce_far(unit, 1)


    def result(self, unit, part, row, size, shift=None):
        layer, edge, piece = self.layer(unit), self.edge, self.piece
        if shift is None:
            first, count = self.core * RING, RING
        else:
            first, count = self.core * RING + self.ring(self.axis(unit, 0), shift), 1
        if self.kind(unit) == OUT:
            return self.r_out.at[layer, pl.ds(first, count), pl.ds(row, size), pl.ds(part * edge, edge)]
        cols = pl.ds(pl.multiple_of(first * piece, piece), count * piece)
        return self.r_in.at[layer, pl.ds(pl.multiple_of(part * edge + row, size), size), cols]

    def shard(self, unit, part):
        row, size = self.span(unit, part, 1, 0)
        return self.wp.at[unit % HELD, pl.ds(part, 1), pl.ds(row, size)] if self.kind(unit) == OUT else self.wp.at[unit % HELD, part, pl.ds(row, size)]

    @once
    def keep(self, unit, part):
        return pltpu.make_async_copy(
            self.shard(unit, part), self.result(unit, part, *self.span(unit, part, 1, 0), 0), self.own_sem.at[unit, part]
        )

    @once
    def ag(self, unit, part, phase, step, way):
        axis, block, half = self.rs_axis(unit, part, 0), 0, None
        if step:
            block, half = self.back(way), way
        if phase == 2:
            src = dst = self.result(unit, part, *self.span(unit, part, 0, block, half))
        elif (phase == 0) == ((unit, part) in CROSSED):
            axis = self.rs_axis(unit, part, 1)
            dst = self.result(unit, part, *self.span(unit, part, 1, block, half), 0 if phase == 0 else None)
            src = dst
        else:
            axis = self.axis(unit, 0)
            dst = self.result(unit, part, *self.span(unit, part, 1 - phase, 0, half), block)
            src = dst
        if phase == 0 and step == 0:
            src = self.shard(unit, part)
        index = 26 + ((part * 3 + phase) * 2 + step) * 2 + way
        return self.copy(unit, index, src, dst, self.device(axis, self.side(way)))

    @once
    def pair(self, unit, part, j):
        block, half = ((0, None), (3, None), (1, None), (2, 0), (2, 1))[j]
        ref = self.result(unit, part, *self.span(unit, part, 0, block, half))
        return self.copy(unit, 50 + part * 5 + j, ref, ref, self.partner())

    def gather_on(self, unit, phase):
        for part in range(2):
            for way in range(2):
                self.ag(unit, part, phase, 0, way).wait_recv()
                self.ag(unit, part, phase, 1, way).start()
                if phase == 2:
                    self.pair(unit, part, 1 + way).start()

    def gather_next(self, unit, phase):
        for part in range(2):
            for way in range(2):
                self.ag(unit, part, phase - 1, 1, way).wait_recv()
            if phase == 1:
                self.keep(unit, part).wait()
            for way in range(2):
                self.ag(unit, part, phase, 0, way).start()
            if phase == 2:
                self.pair(unit, part, 0).start()

    def gather_1(self, unit):
        self.gather_on(unit, 0)

    def gather_2(self, unit):
        self.gather_next(unit, 1)

    def gather_3(self, unit):
        self.gather_on(unit, 1)

    def gather_4(self, unit):
        self.gather_next(unit, 2)

    def gather_5(self, unit):
        self.gather_on(unit, 2)

    def gather_6(self, unit):
        for part in range(2):
            for way in range(2):
                self.ag(unit, part, 2, 1, way).wait_recv()
                self.pair(unit, part, 3 + way).start()

    def sent(self, unit):
        for part in range(2):
            for way in range(2):
                for step in range(2):
                    for phase in range(2):
                        self.rs(unit, part, phase, step, way).wait_send()
                self.ag(unit, part, 0, 0, way).wait_send()

    def finish(self, unit):
        if unit + HELD >= 2 * self.layers:
            self.sent(unit)
        for part in range(2):
            for j in range(5):
                self.pair(unit, part, j).wait()
            for way in range(2):
                self.ag(unit, part, 0, 1, way).wait_send()
                for step in range(2):
                    for phase in (1, 2):
                        self.ag(unit, part, phase, step, way).wait_send()
        for way in range(2):
            for later in range(2):
                self.full_out(unit, way, later).wait_send()
            self.full_on(unit, way).wait_send()
        for j in range(4):
            self.full_pair(unit, j).wait_send()

    def meet(self):
        barrier = pltpu.get_barrier_semaphore()
        others = [self.device(axis, shift) for axis in range(3) for shift in (1, 3)] + [self.partner()]
        for other in others:
            pl.semaphore_signal(barrier, inc=1, device_id=other, device_id_type=MESH)
        pl.semaphore_wait(barrier, len(others))

    def run(self):
        units = range(2 * self.layers)
        self.ahead(0, True)
        self.move(self.tokens, self.cur)
        self.meet()
        for code in ORDER:
            stage, unit = STAGES[code // 10], code % 10
            if unit < (self.layers if code < 20 else 2 * self.layers):
                getattr(self, stage)(unit)
        for unit in units:
            self.finish(unit)


def weight_grads(tokens, targets, w_in, w_out, inv_total):
    toks, dim = tokens.shape
    layers, _, hid = w_in.shape
    units, edge, piece, tile = 2 * layers, dim // 2, hid // 8, min(512, hid // 2)
    slots = min(4, hid // tile)
    assert edge == piece
    block, small = edge // RING, edge // RING**2

    def body(*refs):
        rest = refs[9:]
        near, far = (rest[4], rest[6]), (rest[5], rest[7])
        Reducer(refs[:4], refs[4:9], (*rest[:4], near, far, *rest[8:]), layers, toks, dim, hid, inv_total).run()

    anywhere = pl.BlockSpec(memory_space=pl.ANY)
    grad_in, grad_out, *_ = pl.pallas_call(
        body,
        in_specs=[anywhere] * 4,
        out_specs=[anywhere] * 5,
        out_shape=[
            jax.ShapeDtypeStruct((layers, dim, hid), F32),
            jax.ShapeDtypeStruct((layers, 8, piece, dim), F32),
            jax.ShapeDtypeStruct((units, 8, toks, dim), BF16),
            jax.ShapeDtypeStruct((layers, toks, dim), BF16),
            jax.ShapeDtypeStruct((layers, toks, dim), BF16),
        ],
        scratch_shapes=[
            pltpu.VMEM((2, 8 * toks, dim), BF16),
            pltpu.VMEM((8 * toks, piece), BF16),
            pltpu.VMEM((8 * toks, piece), BF16),
            pltpu.VMEM((min(HELD, units), 2, edge, edge), F32),
            pltpu.VMEM((units, 2, 2, block // 2, edge), F32),
            pltpu.VMEM((units, 2, 2, block, edge), F32),
            pltpu.VMEM((units, 2, 2, small // 2, edge), F32),
            pltpu.VMEM((units, 2, 2, small, edge), F32),
            pltpu.SemaphoreType.DMA((2, units, 60)),
            pltpu.SemaphoreType.DMA((2, 8)),
            pltpu.SemaphoreType.DMA((units + 1, 2)),
            pltpu.VMEM((toks, dim), BF16),
            pltpu.VMEM((toks, dim), F32),
            pltpu.VMEM((layers, toks, hid), BF16),
            pltpu.VMEM((slots, dim, tile), BF16),
            pltpu.VMEM((slots, tile, dim), BF16),
            pltpu.SemaphoreType.DMA((slots, 2)),
            pltpu.VMEM((dim, piece), BF16),
            pltpu.VMEM((piece, dim), BF16),
            pltpu.SemaphoreType.DMA((2,)),
        ],
        compiler_params=pltpu.CompilerParams(collective_id=1, has_side_effects=True, vmem_limit_bytes=63 << 20),
        cost_estimate=pl.CostEstimate(
            flops=16 * layers * toks * dim * hid, bytes_accessed=40 * layers * dim * hid, transcendentals=2 * layers * toks * hid
        ),
        name='weight_grads',
    )(tokens, targets, w_in, w_out)
    return grad_in, grad_out.reshape(layers, hid, dim)


def settle(arrays):
    blocks, ahead = 32, 4
    slots = 2 * ahead
    count = len(arrays)
    flat = [array.reshape(blocks, -1, array.shape[-1]) for array in arrays]

    def body(*refs):
        src, dst, held, sems = refs[:count], refs[count : 2 * count], refs[2 * count : 3 * count], refs[-1]

        def reads(i):
            slot = lax.rem(i, slots)
            return [pltpu.make_async_copy(src[k].at[i], held[k].at[slot], sems.at[0, k, slot]) for k in range(count)]

        def writes(i):
            slot = lax.rem(i, slots)
            return [pltpu.make_async_copy(held[k].at[slot], dst[k].at[i], sems.at[1, k, slot]) for k in range(count)]

        def step(i, carry):
            for read, write in zip(reads(i), writes(i)):
                read.wait()
                write.start()

            @pl.when((i >= ahead) & (i + ahead < blocks))
            def _():
                for write in writes(i - ahead):
                    write.wait()

            @pl.when(i + ahead < blocks)
            def _():
                for read in reads(i + ahead):
                    read.start()

            return carry

        def last(i, carry):
            for write in writes(i):
                write.wait()
            return carry

        for i in range(ahead):
            for read in reads(i):
                read.start()
        lax.fori_loop(0, blocks, step, 0)
        lax.fori_loop(blocks - slots, blocks, last, 0)

    anywhere = pl.BlockSpec(memory_space=pl.ANY)
    size = sum(array.size for array in arrays)
    out = pl.pallas_call(
        body,
        in_specs=[anywhere] * count,
        out_specs=[anywhere] * count,
        out_shape=[jax.ShapeDtypeStruct(x.shape, x.dtype) for x in flat],
        scratch_shapes=[pltpu.VMEM((slots, *x.shape[1:]), x.dtype) for x in flat] + [pltpu.SemaphoreType.DMA((2, count, slots))],
        compiler_params=pltpu.CompilerParams(vmem_limit_bytes=48 << 20),
        cost_estimate=pl.CostEstimate(flops=size, bytes_accessed=8 * size, transcendentals=0),
        name='settle',
    )(*flat)
    return [x.reshape(array.shape) for x, array in zip(out, arrays)]


def solution(mesh):
    def run(tokens, targets, w_in, w_out):
        inv_total = 1.0 / tokens.shape[0]

        def local_step(tok_local, tgt_local, w_first_all, w_second_all):
            return tuple(settle(weight_grads(tok_local, tgt_local, w_first_all, w_second_all, inv_total)))

        data_spec = P(DATA_AXES, None)
        mapped = jax.shard_map(local_step, mesh=mesh, in_specs=(data_spec, data_spec, P(), P()), out_specs=(P(), P()), check_vma=False)
        return mapped(tokens, targets, w_in, w_out)

    return run
```

```python
import functools

import jax
import jax.numpy as jnp
from jax import lax
from jax.experimental import pallas as pl
from jax.experimental.pallas import tpu as pltpu
from jax.sharding import PartitionSpec as P

DATA_AXES = ('dy', 'dx')
MESH = pl.DeviceIdType.MESH
RING = 4
ROW_CONTRACT = (((0,), (0,)), ((), ()))
COL_CONTRACT = (((1,), (1,)), ((), ()))
F32, BF16 = jnp.float32, jnp.bfloat16


SCALE, CUBIC = 0.7978845608028654, 0.044715
OUT, IN = 0, 1
HELD = 5
STAGES = (
    'forward',
    'backward',
    'swap_full',
    'full_2',
    'full_3',
    'load',
    'again',
    'product',
    'reduce_2',
    'reduce_3',
    'reduce_4',
    'reduce_5',
    'gather_1',
    'gather_2',
    'gather_3',
    'gather_4',
    'gather_5',
    'gather_6',
)
ORDER = (
    0, 27, 1, 2, 21, 23, 3, 20, 13, 22, 31, 33, 25, 12, 32, 24, 30, 11, 41, 35,
    37, 40, 43, 51, 26, 42, 34, 50, 61, 70, 71, 53, 80, 36, 52, 44, 63, 45, 81, 72,
    90, 73, 54, 55, 91, 100, 82, 65, 101, 110, 74, 92, 120, 111, 46, 102, 84, 121, 47, 130,
    112, 75, 57, 56, 83, 122, 131, 67, 76, 85, 132, 77, 86, 93, 94, 95, 87, 96, 105, 142,
    103, 104, 97, 141, 106, 115, 107, 140, 113, 116, 117, 123, 125, 114, 150, 126, 133, 127, 152, 124,
    135, 10, 160, 145, 151, 155, 137, 147, 134, 143, 157, 144, 161, 136, 146, 156, 153, 162, 165, 170,
    154, 171, 167, 163, 175, 166, 164, 177, 172, 173, 176, 174,
)
CROSSED = ((0, 1), (1, 0), (6, 0), (6, 1), (7, 0), (7, 1))


def gate(x):
    square = x * x
    return jnp.tanh(x * (SCALE + SCALE * CUBIC * square)), square


def gelu(x):
    tanh, _ = gate(x)
    return x * (0.5 + 0.5 * tanh)


def gelu_slope(x):
    tanh, square = gate(x)
    return 0.5 + 0.5 * tanh + (0.5 - 0.5 * tanh * tanh) * x * (SCALE + 3 * SCALE * CUBIC * square)


def once(method):
    @functools.wraps(method)
    def get(self, *args):
        key = method.__name__, args
        if key not in self.memo:
            self.memo[key] = method(self, *args)
        return self.memo[key]

    return get


class Reducer:
    def __init__(self, ins, outs, scratch, layers, toks, dim, hid, inv_total):
        self.tokens, self.targets, self.w_in, self.w_out = ins
        self.r_in, self.r_out, self.fx, self.h, self.g = outs
        self.fbuf, self.ubuf, self.sbuf, self.wp, self.near, self.far, self.sems, self.load_sem, self.own_sem, *local = scratch
        self.cur, self.acc, self.pre, self.w1, self.w2, self.w_sem, self.v1, self.v2, self.v_sem = local
        self.tile, self.slots = self.w1.shape[-1], self.w1.shape[0]
        self.tiles = hid // self.tile
        self.layers, self.toks, self.dim, self.hid = layers, toks, dim, hid
        self.memo = {}
        self.unsaved = None
        self.inv_total = inv_total
        self.piece, self.edge = hid // 8, dim // 2
        dx = lax.axis_index('dx')
        self.core = lax.rem(dx, 2)
        self.at = (lax.axis_index('dy'), lax.rem(lax.div(dx, 2), RING), lax.div(dx, 2 * RING))

    def kind(self, unit):
        return unit % 2

    def layer(self, unit):
        return self.layers - 1 - unit // 2

    def axis(self, unit, k):
        return (unit // 2 + k) % 3

    @once
    def ring(self, axis, shift):
        return lax.rem(self.at[axis] + shift, RING)

    @once
    def chip(self, axis, shift):
        x, y, z = (self.ring(i, shift) if i == axis else c for i, c in enumerate(self.at))
        return x, (z * RING + y) * 2

    @once
    def device(self, axis, shift, core=None):
        x, rest = self.chip(axis, shift)
        return x, rest + (self.core if core is None else core)

    @once
    def partner(self):
        x, rest = self.chip(None, 0)
        return x, rest + (1 - self.core)

    def copy(self, unit, index, src, dst, device, recv_index=None):
        recv = index if recv_index is None else recv_index
        return pltpu.make_async_remote_copy(
            src, dst, self.sems.at[0, unit, index], self.sems.at[1, unit, recv], device_id=device, device_id_type=MESH
        )


    def move(self, src, dst):
        copy = pltpu.make_async_copy(src, dst, self.own_sem.at[2 * self.layers, 0])
        copy.start()
        copy.wait()

    def save(self, place):
        self.unsaved = pltpu.make_async_copy(self.cur, place, self.own_sem.at[2 * self.layers, 1])
        self.unsaved.start()

    def saved(self):
        if self.unsaved is not None:
            self.unsaved.wait()
            self.unsaved = None

    def fetch(self, layer, tile, first):
        part, slot = pl.ds(pl.multiple_of(tile * self.tile, self.tile), self.tile), lax.rem(tile, self.slots)
        copies = [pltpu.make_async_copy(self.w_out.at[layer, part], self.w2.at[slot], self.w_sem.at[slot, 1])]
        if first:
            copies.append(pltpu.make_async_copy(self.w_in.at[layer, :, part], self.w1.at[slot], self.w_sem.at[slot, 0]))
        return copies

    def ahead(self, layer, first):
        for tile in range(self.slots - 1):
            for copy in self.fetch(layer, tile, first):
                copy.start()

    def over_tiles(self, layer, first, following, work):
        tiles = self.tiles

        def step(tile, carry):
            for copy in self.fetch(layer, tile, first):
                copy.wait()
            later = tile + self.slots - 1

            @pl.when(later < tiles)
            def _():
                for copy in self.fetch(layer, later, first):
                    copy.start()

            if following is not None:

                @pl.when(later >= tiles)
                def _():
                    for copy in self.fetch(following[0], later - tiles, following[1]):
                        copy.start()

            work(lax.rem(tile, self.slots), pl.ds(pl.multiple_of(tile * self.tile, self.tile), self.tile))
            return carry

        lax.fori_loop(0, tiles, step, 0)

    def forward(self, layer):
        top = self.layers - 1

        def work(slot, part):
            pre_act = jnp.dot(self.cur[:, :], self.w1[slot], preferred_element_type=F32).astype(BF16)
            self.pre[layer, :, part] = pre_act
            post_act = gelu(pre_act.astype(F32)).astype(BF16)
            self.acc[:, :] += jnp.dot(post_act, self.w2[slot], preferred_element_type=F32)

        self.acc[:, :] = self.cur[:, :].astype(F32)
        following = (layer + 1, True) if layer < top else ((top, True) if top > 0 else None)
        self.over_tiles(layer, True, following, work)
        self.saved()
        self.cur[:, :] = self.acc[:, :].astype(BF16)
        if layer == top:
            targets = self.fbuf.at[0, pl.ds(0, self.toks)]
            self.move(self.targets, targets)
            gap = self.cur[:, :].astype(F32) - targets[:, :].astype(F32)
            self.cur[:, :] = (gap * self.inv_total).astype(BF16)
        self.save(self.h.at[layer + 1] if layer < top else self.g.at[top])

    def backward(self, layer):
        def work(slot, part):
            grad_post = lax.dot_general(self.cur[:, :], self.w2[slot], COL_CONTRACT, preferred_element_type=F32)
            pre_act = self.pre[layer, :, part].astype(F32)
            grad_pre = (grad_post * gelu_slope(pre_act)).astype(BF16)
            self.acc[:, :] += lax.dot_general(grad_pre, self.w1[slot], COL_CONTRACT, preferred_element_type=F32)

        if layer > 0:
            self.acc[:, :] = self.cur[:, :].astype(F32)
            self.over_tiles(layer, True, (layer - 1, True) if layer > 1 else None, work)
            self.saved()
            self.cur[:, :] = self.acc[:, :].astype(BF16)
            self.save(self.g.at[layer - 1])


    def full(self, unit):
        layer = self.layer(unit)
        if self.kind(unit) == IN and layer == 0:
            return self.tokens
        return (self.g, self.h)[self.kind(unit)].at[layer]

    def side(self, way):
        return 1 + 2 * way

    def back(self, way):
        return RING - self.side(way)

    def half(self, way):
        return way * (self.toks // 2), self.toks // 2

    @once
    def slot(self, unit, shift, other=0):
        return self.ring(self.axis(unit, 0), shift) * 2 + (1 - self.core if other else self.core)

    @once
    def full_out(self, unit, way, later):
        rows = pl.ds(*self.half(1 - way if later else way))
        dst = self.fx.at[unit, self.slot(unit, 0), rows]
        return self.copy(unit, 2 * later + way, self.full(unit).at[rows], dst, self.device(self.axis(unit, 0), self.side(way)))

    @once
    def full_on(self, unit, way):
        ref = self.fx.at[unit, self.slot(unit, self.back(way)), pl.ds(*self.half(way))]
        return self.copy(unit, 4 + way, ref, ref, self.device(self.axis(unit, 0), self.side(way)))

    @once
    def full_pair(self, unit, j):
        ref = self.fx.at[unit, self.slot(unit, (0, 3, 1, 2)[j])]
        return self.copy(unit, 6 + j, self.full(unit) if j == 0 else ref, ref, self.partner())

    def swap_full(self, unit):
        self.saved()
        for later in range(2):
            for way in range(2):
                self.full_out(unit, way, later).start()
        self.full_pair(unit, 0).start()

    def full_2(self, unit):
        for way in range(2):
            self.full_out(unit, way, 0).wait_recv()
            self.full_on(unit, way).start()

    def full_3(self, unit):
        for way in range(2):
            self.full_out(unit, way, 1).wait_recv()
            self.full_pair(unit, 1 + way).start()
        for way in range(2):
            self.full_on(unit, way).wait_recv()
        self.full_pair(unit, 3).start()


    @once
    def loads(self, unit):
        kind, layer, copies = self.kind(unit), self.layer(unit), []
        for j in range(8):
            src = self.fx.at[unit, self.slot(unit, j // 2, j % 2)] if j else self.full(unit)
            copies.append(pltpu.make_async_copy(src, self.fbuf.at[kind, pl.ds(j * self.toks, self.toks)], self.load_sem.at[kind, j]))
        if kind == IN:
            place = self.core * RING + self.at[self.axis(unit, 0)]
            share = pl.ds(pl.multiple_of(place * self.piece, self.piece), self.piece)
            copies.append(pltpu.make_async_copy(self.w_in.at[layer, :, share], self.v1, self.v_sem.at[0]))
            copies.append(pltpu.make_async_copy(self.w_out.at[layer, share], self.v2, self.v_sem.at[1]))
        return copies

    def load(self, unit):
        for j in range(4):
            self.full_pair(unit, j).wait_recv()
        for copy in self.loads(unit):
            copy.start()

    def again(self, unit):
        for copy in self.loads(unit):
            copy.wait()
        self.over_rows(self.again_rows)

    def over_rows(self, work):
        def step(j, carry):
            work(pl.ds(pl.multiple_of(j * self.toks, self.toks), self.toks))
            return carry

        lax.fori_loop(0, 8, step, 0)

    def again_rows(self, rows):
        pre_act = jnp.dot(self.fbuf[1, rows], self.v1[:, :], preferred_element_type=F32).astype(BF16)
        self.ubuf[rows, :] = pre_act
        self.sbuf[rows, :] = gelu(pre_act.astype(F32)).astype(BF16)

    def again_back(self, rows):
        grad_post = lax.dot_general(self.fbuf[0, rows], self.v2[:, :], COL_CONTRACT, preferred_element_type=F32)
        pre_act = self.ubuf[rows, :].astype(F32)
        self.sbuf[rows, :] = (grad_post * gelu_slope(pre_act)).astype(BF16)

    def product(self, unit):
        if unit >= HELD:
            self.sent(unit - HELD)
        if self.kind(unit) == OUT:
            for copy in self.loads(unit):
                copy.wait()
        else:
            self.over_rows(self.again_back)
        sbuf, wp, edge = self.sbuf, self.wp.at[unit % HELD], self.edge
        block = edge // 2

        def step(b, carry):
            rows = pl.ds(pl.multiple_of(b * block, block), block)
            if self.kind(unit) == OUT:
                for part in range(2):
                    grads = self.fbuf[0, :, pl.ds(part * edge, edge)]
                    wp[part, rows] = lax.dot_general(sbuf[:, rows], grads, ROW_CONTRACT, preferred_element_type=F32)
            else:
                term = lax.dot_general(self.fbuf[1, :, rows], sbuf[:, :], ROW_CONTRACT, preferred_element_type=F32)
                wp[lax.div(b, 2), pl.ds(pl.multiple_of(lax.rem(b, 2) * block, block), block)] = term
            return carry

        lax.fori_loop(0, 2 if self.kind(unit) == OUT else 4, step, 0)
        for part in range(2):
            for way in range(2):
                self.rs(unit, part, 0, 0, way).start()


    def rs_axis(self, unit, part, phase):
        return self.axis(unit, 1 + (part + phase) % 2)

    @once
    def span(self, unit, part, phase, block, half=None):
        size = self.edge // RING
        base = 0
        if phase:
            base = self.at[self.rs_axis(unit, part, 0)] * size
            size //= RING
        row = base + self.ring(self.rs_axis(unit, part, phase), block) * size
        if half is not None:
            size //= 2
            row = row + half * size
        return pl.multiple_of(row, size), size

    @once
    def rs(self, unit, part, phase, step, way):
        if step == 0:
            row, size = self.span(unit, part, phase, 2, way)
            dst = self.near[phase]
        else:
            row, size = self.span(unit, part, phase, self.side(way))
            dst = self.far[phase]
        index = 10 + ((part * 2 + phase) * 2 + step) * 2 + way
        src = self.wp.at[unit % HELD, part, pl.ds(row, size)]
        return self.copy(unit, index, src, dst.at[unit, part, way], self.device(self.rs_axis(unit, part, phase), self.side(way)))

    def accumulate(self, unit, part, row, size, sources):
        chunk = min(16, size)

        def step(i, carry):
            at = pl.multiple_of(i * chunk, chunk)
            here = pl.ds(pl.multiple_of(row + at, chunk), chunk)
            total = self.wp[unit % HELD, part, here]
            for ref, way in sources:
                total = total + ref[unit, part, way, pl.ds(at, chunk)]
            self.wp[unit % HELD, part, here] = total
            return carry

        lax.fori_loop(0, size // chunk, step, 0)

    def reduce_near(self, unit, phase):
        for part in range(2):
            for way in range(2):
                self.rs(unit, part, phase, 0, way).wait_recv()
                row, size = self.span(unit, part, phase, self.side(way), way)
                self.accumulate(unit, part, row, size, [(self.near[phase], way)])
                self.rs(unit, part, phase, 1, way).start()

    def reduce_far(self, unit, phase):
        for part in range(2):
            for way in range(2):
                self.rs(unit, part, phase, 1, way).wait_recv()
            row, size = self.span(unit, part, phase, 0)
            self.accumulate(unit, part, row, size, [(self.far[phase], 0), (self.far[phase], 1)])
            for way in range(2):
                if phase == 0:
                    self.rs(unit, part, 1, 0, way).start()
                else:
                    self.ag(unit, part, 0, 0, way).start()
            if phase == 1:
                self.keep(unit, part).start()

    def reduce_2(self, unit):
        self.reduce_near(unit, 0)

    def reduce_3(self, unit):
        self.reduce_far(unit, 0)

    def reduce_4(self, unit):
        self.reduce_near(unit, 1)

    def reduce_5(self, unit):
        self.reduce_far(unit, 1)


    def result(self, unit, part, row, size, shift=None):
        layer, edge, piece = self.layer(unit), self.edge, self.piece
        if shift is None:
            first, count = self.core * RING, RING
        else:
            first, count = self.core * RING + self.ring(self.axis(unit, 0), shift), 1
        if self.kind(unit) == OUT:
            return self.r_out.at[layer, pl.ds(first, count), pl.ds(row, size), pl.ds(part * edge, edge)]
        cols = pl.ds(pl.multiple_of(first * piece, piece), count * piece)
        return self.r_in.at[layer, pl.ds(pl.multiple_of(part * edge + row, size), size), cols]

    def shard(self, unit, part):
        row, size = self.span(unit, part, 1, 0)
        return self.wp.at[unit % HELD, pl.ds(part, 1), pl.ds(row, size)] if self.kind(unit) == OUT else self.wp.at[unit % HELD, part, pl.ds(row, size)]

    @once
    def keep(self, unit, part):
        return pltpu.make_async_copy(
            self.shard(unit, part), self.result(unit, part, *self.span(unit, part, 1, 0), 0), self.own_sem.at[unit, part]
        )

    @once
    def ag(self, unit, part, phase, step, way):
        axis, block, half = self.rs_axis(unit, part, 0), 0, None
        if step:
            block, half = self.back(way), way
        if phase == 2:
            src = dst = self.result(unit, part, *self.span(unit, part, 0, block, half))
        elif (phase == 0) == ((unit, part) in CROSSED):
            axis = self.rs_axis(unit, part, 1)
            dst = self.result(unit, part, *self.span(unit, part, 1, block, half), 0 if phase == 0 else None)
            src = dst
        else:
            axis = self.axis(unit, 0)
            dst = self.result(unit, part, *self.span(unit, part, 1 - phase, 0, half), block)
            src = dst
        if phase == 0 and step == 0:
            src = self.shard(unit, part)
        index = 26 + ((part * 3 + phase) * 2 + step) * 2 + way
        return self.copy(unit, index, src, dst, self.device(axis, self.side(way)))

    @once
    def pair(self, unit, part, j):
        block, half = ((0, None), (3, None), (1, None), (2, 0), (2, 1))[j]
        ref = self.result(unit, part, *self.span(unit, part, 0, block, half))
        return self.copy(unit, 50 + part * 5 + j, ref, ref, self.partner())

    def gather_on(self, unit, phase):
        for part in range(2):
            for way in range(2):
                self.ag(unit, part, phase, 0, way).wait_recv()
                self.ag(unit, part, phase, 1, way).start()
                if phase == 2:
                    self.pair(unit, part, 1 + way).start()

    def gather_next(self, unit, phase):
        for part in range(2):
            for way in range(2):
                self.ag(unit, part, phase - 1, 1, way).wait_recv()
            if phase == 1:
                self.keep(unit, part).wait()
            for way in range(2):
                self.ag(unit, part, phase, 0, way).start()
            if phase == 2:
                self.pair(unit, part, 0).start()

    def gather_1(self, unit):
        self.gather_on(unit, 0)

    def gather_2(self, unit):
        self.gather_next(unit, 1)

    def gather_3(self, unit):
        self.gather_on(unit, 1)

    def gather_4(self, unit):
        self.gather_next(unit, 2)

    def gather_5(self, unit):
        self.gather_on(unit, 2)

    def gather_6(self, unit):
        for part in range(2):
            for way in range(2):
                self.ag(unit, part, 2, 1, way).wait_recv()
                self.pair(unit, part, 3 + way).start()

    def sent(self, unit):
        for part in range(2):
            for way in range(2):
                for step in range(2):
                    for phase in range(2):
                        self.rs(unit, part, phase, step, way).wait_send()
                self.ag(unit, part, 0, 0, way).wait_send()

    def finish(self, unit):
        if unit + HELD >= 2 * self.layers:
            self.sent(unit)
        for part in range(2):
            for j in range(5):
                self.pair(unit, part, j).wait()
            for way in range(2):
                self.ag(unit, part, 0, 1, way).wait_send()
                for step in range(2):
                    for phase in (1, 2):
                        self.ag(unit, part, phase, step, way).wait_send()
        for way in range(2):
            for later in range(2):
                self.full_out(unit, way, later).wait_send()
            self.full_on(unit, way).wait_send()
        for j in range(4):
            self.full_pair(unit, j).wait_send()

    def meet(self):
        barrier = pltpu.get_barrier_semaphore()
        others = [self.device(axis, shift) for axis in range(3) for shift in (1, 3)] + [self.partner()]
        for other in others:
            pl.semaphore_signal(barrier, inc=1, device_id=other, device_id_type=MESH)
        pl.semaphore_wait(barrier, len(others))

    def run(self):
        units = range(2 * self.layers)
        self.ahead(0, True)
        self.move(self.tokens, self.cur)
        self.meet()
        for code in ORDER:
            stage, unit = STAGES[code // 10], code % 10
            if unit < (self.layers if code < 20 else 2 * self.layers):
                getattr(self, stage)(unit)
        for unit in units:
            self.finish(unit)


def weight_grads(tokens, targets, w_in, w_out, inv_total):
    toks, dim = tokens.shape
    layers, _, hid = w_in.shape
    units, edge, piece, tile = 2 * layers, dim // 2, hid // 8, min(512, hid // 2)
    slots = min(4, hid // tile)
    assert edge == piece
    block, small = edge // RING, edge // RING**2

    def body(*refs):
        rest = refs[9:]
        near, far = (rest[4], rest[6]), (rest[5], rest[7])
        Reducer(refs[:4], refs[4:9], (*rest[:4], near, far, *rest[8:]), layers, toks, dim, hid, inv_total).run()

    anywhere = pl.BlockSpec(memory_space=pl.ANY)
    grad_in, grad_out, *_ = pl.pallas_call(
        body,
        in_specs=[anywhere] * 4,
        out_specs=[anywhere] * 5,
        out_shape=[
            jax.ShapeDtypeStruct((layers, dim, hid), F32),
            jax.ShapeDtypeStruct((layers, 8, piece, dim), F32),
            jax.ShapeDtypeStruct((units, 8, toks, dim), BF16),
            jax.ShapeDtypeStruct((layers, toks, dim), BF16),
            jax.ShapeDtypeStruct((layers, toks, dim), BF16),
        ],
        scratch_shapes=[
            pltpu.VMEM((2, 8 * toks, dim), BF16),
            pltpu.VMEM((8 * toks, piece), BF16),
            pltpu.VMEM((8 * toks, piece), BF16),
            pltpu.VMEM((min(HELD, units), 2, edge, edge), F32),
            pltpu.VMEM((units, 2, 2, block // 2, edge), F32),
            pltpu.VMEM((units, 2, 2, block, edge), F32),
            pltpu.VMEM((units, 2, 2, small // 2, edge), F32),
            pltpu.VMEM((units, 2, 2, small, edge), F32),
            pltpu.SemaphoreType.DMA((2, units, 60)),
            pltpu.SemaphoreType.DMA((2, 8)),
            pltpu.SemaphoreType.DMA((units + 1, 2)),
            pltpu.VMEM((toks, dim), BF16),
            pltpu.VMEM((toks, dim), F32),
            pltpu.VMEM((layers, toks, hid), BF16),
            pltpu.VMEM((slots, dim, tile), BF16),
            pltpu.VMEM((slots, tile, dim), BF16),
            pltpu.SemaphoreType.DMA((slots, 2)),
            pltpu.VMEM((dim, piece), BF16),
            pltpu.VMEM((piece, dim), BF16),
            pltpu.SemaphoreType.DMA((2,)),
        ],
        compiler_params=pltpu.CompilerParams(collective_id=1, has_side_effects=True, vmem_limit_bytes=63 << 20),
        cost_estimate=pl.CostEstimate(
            flops=16 * layers * toks * dim * hid, bytes_accessed=40 * layers * dim * hid, transcendentals=2 * layers * toks * hid
        ),
        name='weight_grads',
    )(tokens, targets, w_in, w_out)
    return grad_in, grad_out.reshape(layers, hid, dim)


def settle(arrays):
    blocks, ahead = 32, 4
    slots = 2 * ahead
    count = len(arrays)
    flat = [array.reshape(blocks, -1, array.shape[-1]) for array in arrays]

    def body(*refs):
        src, dst, held, sems = refs[:count], refs[count : 2 * count], refs[2 * count : 3 * count], refs[-1]

        def reads(i):
            slot = lax.rem(i, slots)
            return [pltpu.make_async_copy(src[k].at[i], held[k].at[slot], sems.at[0, k, slot]) for k in range(count)]

        def writes(i):
            slot = lax.rem(i, slots)
            return [pltpu.make_async_copy(held[k].at[slot], dst[k].at[i], sems.at[1, k, slot]) for k in range(count)]

        def step(i, carry):
            for read, write in zip(reads(i), writes(i)):
                read.wait()
                write.start()

            @pl.when((i >= ahead) & (i + ahead < blocks))
            def _():
                for write in writes(i - ahead):
                    write.wait()

            @pl.when(i + ahead < blocks)
            def _():
                for read in reads(i + ahead):
                    read.start()

            return carry

        def last(i, carry):
            for write in writes(i):
                write.wait()
            return carry

        for i in range(ahead):
            for read in reads(i):
                read.start()
        lax.fori_loop(0, blocks, step, 0)
        lax.fori_loop(blocks - slots, blocks, last, 0)

    anywhere = pl.BlockSpec(memory_space=pl.ANY)
    size = sum(array.size for array in arrays)
    out = pl.pallas_call(
        body,
        in_specs=[anywhere] * count,
        out_specs=[anywhere] * count,
        out_shape=[jax.ShapeDtypeStruct(x.shape, x.dtype) for x in flat],
        scratch_shapes=[pltpu.VMEM((slots, *x.shape[1:]), x.dtype) for x in flat] + [pltpu.SemaphoreType.DMA((2, count, slots))],
        compiler_params=pltpu.CompilerParams(vmem_limit_bytes=48 << 20),
        cost_estimate=pl.CostEstimate(flops=size, bytes_accessed=8 * size, transcendentals=0),
        name='settle',
    )(*flat)
    return [x.reshape(array.shape) for x, array in zip(out, arrays)]


def solution(mesh):
    def run(tokens, targets, w_in, w_out):
        inv_total = 1.0 / tokens.shape[0]

        def local_step(tok_local, tgt_local, w_first_all, w_second_all):
            return tuple(settle(weight_grads(tok_local, tgt_local, w_first_all, w_second_all, inv_total)))

        data_spec = P(DATA_AXES, None)
        mapped = jax.shard_map(local_step, mesh=mesh, in_specs=(data_spec, data_spec, P(), P()), out_specs=(P(), P()), check_vma=False)
        return mapped(tokens, targets, w_in, w_out)

    return run
```

```python
import functools

import jax
import jax.numpy as jnp
from jax import lax
from jax.experimental import pallas as pl
from jax.experimental.pallas import tpu as pltpu
from jax.sharding import PartitionSpec as P

DATA_AXES = ('dy', 'dx')
MESH = pl.DeviceIdType.MESH
RING = 4
ROW_CONTRACT = (((0,), (0,)), ((), ()))
COL_CONTRACT = (((1,), (1,)), ((), ()))
F32, BF16 = jnp.float32, jnp.bfloat16


SCALE, CUBIC = 0.7978845608028654, 0.044715
OUT, IN = 0, 1
HELD = 5
STAGES = (
    'forward',
    'backward',
    'swap_full',
    'full_2',
    'full_3',
    'load',
    'again',
    'product',
    'reduce_2',
    'reduce_3',
    'reduce_4',
    'reduce_5',
    'gather_1',
    'gather_2',
    'gather_3',
    'gather_4',
    'gather_5',
    'gather_6',
)
ORDER = (
    0, 1, 2, 21, 23, 3, 25, 31, 13, 22, 20, 12, 24, 32, 33, 41, 30, 11, 51, 26,
    35, 40, 34, 61, 50, 43, 27, 42, 36, 70, 71, 53, 45, 37, 52, 80, 63, 44, 81, 72,
    90, 73, 54, 55, 91, 100, 82, 65, 101, 110, 74, 92, 120, 111, 102, 84, 47, 46, 10, 130,
    112, 75, 56, 57, 94, 121, 122, 83, 140, 85, 67, 104, 131, 76, 132, 77, 95, 114, 93, 86,
    87, 142, 103, 141, 124, 96, 150, 97, 134, 106, 152, 113, 144, 107, 105, 116, 160, 154, 123, 115,
    126, 162, 117, 125, 151, 136, 146, 133, 135, 161, 145, 164, 127, 143, 156, 137, 174, 147, 153, 157,
    166, 172, 155, 170, 171, 163, 167, 176, 165, 173, 177, 175,
)
CROSSED = ((0, 1), (1, 0), (6, 0), (6, 1), (7, 0), (7, 1))


def gate(x):
    square = x * x
    return jnp.tanh(x * (SCALE + SCALE * CUBIC * square)), square


def gelu(x):
    tanh, _ = gate(x)
    return x * (0.5 + 0.5 * tanh)


def gelu_slope(x):
    tanh, square = gate(x)
    return 0.5 + 0.5 * tanh + (0.5 - 0.5 * tanh * tanh) * x * (SCALE + 3 * SCALE * CUBIC * square)


def once(method):
    @functools.wraps(method)
    def get(self, *args):
        key = method.__name__, args
        if key not in self.memo:
            self.memo[key] = method(self, *args)
        return self.memo[key]

    return get


class Reducer:
    def __init__(self, ins, outs, scratch, layers, toks, dim, hid, inv_total):
        self.tokens, self.targets, self.w_in, self.w_out = ins
        self.r_in, self.r_out, self.fx, self.h, self.g = outs
        self.fbuf, self.ubuf, self.sbuf, self.wp, self.near, self.far, self.sems, self.load_sem, self.own_sem, *local = scratch
        self.cur, self.acc, self.pre, self.w1, self.w2, self.w_sem, self.v1, self.v2, self.v_sem = local
        self.tile, self.slots = self.w1.shape[-1], self.w1.shape[0]
        self.tiles = hid // self.tile
        self.layers, self.toks, self.dim, self.hid = layers, toks, dim, hid
        self.memo = {}
        self.unsaved = None
        self.inv_total = inv_total
        self.piece, self.edge = hid // 8, dim // 2
        dx = lax.axis_index('dx')
        self.core = lax.rem(dx, 2)
        self.at = (lax.axis_index('dy'), lax.rem(lax.div(dx, 2), RING), lax.div(dx, 2 * RING))

    def kind(self, unit):
        return unit % 2

    def layer(self, unit):
        return self.layers - 1 - unit // 2

    def axis(self, unit, k):
        return (unit // 2 + k) % 3

    @once
    def ring(self, axis, shift):
        return lax.rem(self.at[axis] + shift, RING)

    @once
    def chip(self, axis, shift):
        x, y, z = (self.ring(i, shift) if i == axis else c for i, c in enumerate(self.at))
        return x, (z * RING + y) * 2

    @once
    def device(self, axis, shift, core=None):
        x, rest = self.chip(axis, shift)
        return x, rest + (self.core if core is None else core)

    @once
    def partner(self):
        x, rest = self.chip(None, 0)
        return x, rest + (1 - self.core)

    def copy(self, unit, index, src, dst, device, recv_index=None):
        recv = index if recv_index is None else recv_index
        return pltpu.make_async_remote_copy(
            src, dst, self.sems.at[0, unit, index], self.sems.at[1, unit, recv], device_id=device, device_id_type=MESH
        )


    def move(self, src, dst):
        copy = pltpu.make_async_copy(src, dst, self.own_sem.at[2 * self.layers, 0])
        copy.start()
        copy.wait()

    def save(self, place):
        self.unsaved = pltpu.make_async_copy(self.cur, place, self.own_sem.at[2 * self.layers, 1])
        self.unsaved.start()

    def saved(self):
        if self.unsaved is not None:
            self.unsaved.wait()
            self.unsaved = None

    def fetch(self, layer, tile, first):
        part, slot = pl.ds(pl.multiple_of(tile * self.tile, self.tile), self.tile), lax.rem(tile, self.slots)
        copies = [pltpu.make_async_copy(self.w_out.at[layer, part], self.w2.at[slot], self.w_sem.at[slot, 1])]
        if first:
            copies.append(pltpu.make_async_copy(self.w_in.at[layer, :, part], self.w1.at[slot], self.w_sem.at[slot, 0]))
        return copies

    def ahead(self, layer, first):
        for tile in range(self.slots - 1):
            for copy in self.fetch(layer, tile, first):
                copy.start()

    def over_tiles(self, layer, first, following, work):
        tiles = self.tiles

        def step(tile, carry):
            for copy in self.fetch(layer, tile, first):
                copy.wait()
            later = tile + self.slots - 1

            @pl.when(later < tiles)
            def _():
                for copy in self.fetch(layer, later, first):
                    copy.start()

            if following is not None:

                @pl.when(later >= tiles)
                def _():
                    for copy in self.fetch(following[0], later - tiles, following[1]):
                        copy.start()

            work(lax.rem(tile, self.slots), pl.ds(pl.multiple_of(tile * self.tile, self.tile), self.tile))
            return carry

        lax.fori_loop(0, tiles, step, 0)

    def forward(self, layer):
        top = self.layers - 1

        def work(slot, part):
            pre_act = jnp.dot(self.cur[:, :], self.w1[slot], preferred_element_type=F32).astype(BF16)
            self.pre[layer, :, part] = pre_act
            post_act = gelu(pre_act.astype(F32)).astype(BF16)
            self.acc[:, :] += jnp.dot(post_act, self.w2[slot], preferred_element_type=F32)

        self.acc[:, :] = self.cur[:, :].astype(F32)
        following = (layer + 1, True) if layer < top else ((top, True) if top > 0 else None)
        self.over_tiles(layer, True, following, work)
        self.saved()
        self.cur[:, :] = self.acc[:, :].astype(BF16)
        if layer == top:
            targets = self.fbuf.at[0, pl.ds(0, self.toks)]
            self.move(self.targets, targets)
            gap = self.cur[:, :].astype(F32) - targets[:, :].astype(F32)
            self.cur[:, :] = (gap * self.inv_total).astype(BF16)
        self.save(self.h.at[layer + 1] if layer < top else self.g.at[top])

    def backward(self, layer):
        def work(slot, part):
            grad_post = lax.dot_general(self.cur[:, :], self.w2[slot], COL_CONTRACT, preferred_element_type=F32)
            pre_act = self.pre[layer, :, part].astype(F32)
            grad_pre = (grad_post * gelu_slope(pre_act)).astype(BF16)
            self.acc[:, :] += lax.dot_general(grad_pre, self.w1[slot], COL_CONTRACT, preferred_element_type=F32)

        if layer > 0:
            self.acc[:, :] = self.cur[:, :].astype(F32)
            self.over_tiles(layer, True, (layer - 1, True) if layer > 1 else None, work)
            self.saved()
            self.cur[:, :] = self.acc[:, :].astype(BF16)
            self.save(self.g.at[layer - 1])


    def full(self, unit):
        layer = self.layer(unit)
        if self.kind(unit) == IN and layer == 0:
            return self.tokens
        return (self.g, self.h)[self.kind(unit)].at[layer]

    def side(self, way):
        return 1 + 2 * way

    def back(self, way):
        return RING - self.side(way)

    def half(self, way):
        return way * (self.toks // 2), self.toks // 2

    @once
    def slot(self, unit, shift, other=0):
        return self.ring(self.axis(unit, 0), shift) * 2 + (1 - self.core if other else self.core)

    @once
    def full_out(self, unit, way, later):
        rows = pl.ds(*self.half(1 - way if later else way))
        dst = self.fx.at[unit, self.slot(unit, 0), rows]
        return self.copy(unit, 2 * later + way, self.full(unit).at[rows], dst, self.device(self.axis(unit, 0), self.side(way)))

    @once
    def full_on(self, unit, way):
        ref = self.fx.at[unit, self.slot(unit, self.back(way)), pl.ds(*self.half(way))]
        return self.copy(unit, 4 + way, ref, ref, self.device(self.axis(unit, 0), self.side(way)))

    @once
    def full_pair(self, unit, j):
        ref = self.fx.at[unit, self.slot(unit, (0, 3, 1, 2)[j])]
        return self.copy(unit, 6 + j, self.full(unit) if j == 0 else ref, ref, self.partner())

    def swap_full(self, unit):
        self.saved()
        for later in range(2):
            for way in range(2):
                self.full_out(unit, way, later).start()
        self.full_pair(unit, 0).start()

    def full_2(self, unit):
        for way in range(2):
            self.full_out(unit, way, 0).wait_recv()
            self.full_on(unit, way).start()

    def full_3(self, unit):
        for way in range(2):
            self.full_out(unit, way, 1).wait_recv()
            self.full_pair(unit, 1 + way).start()
        for way in range(2):
            self.full_on(unit, way).wait_recv()
        self.full_pair(unit, 3).start()


    @once
    def loads(self, unit):
        kind, layer, copies = self.kind(unit), self.layer(unit), []
        for j in range(8):
            src = self.fx.at[unit, self.slot(unit, j // 2, j % 2)] if j else self.full(unit)
            copies.append(pltpu.make_async_copy(src, self.fbuf.at[kind, pl.ds(j * self.toks, self.toks)], self.load_sem.at[kind, j]))
        if kind == IN:
            place = self.core * RING + self.at[self.axis(unit, 0)]
            share = pl.ds(pl.multiple_of(place * self.piece, self.piece), self.piece)
            copies.append(pltpu.make_async_copy(self.w_in.at[layer, :, share], self.v1, self.v_sem.at[0]))
            copies.append(pltpu.make_async_copy(self.w_out.at[layer, share], self.v2, self.v_sem.at[1]))
        return copies

    def load(self, unit):
        for j in range(4):
            self.full_pair(unit, j).wait_recv()
        for copy in self.loads(unit):
            copy.start()

    def again(self, unit):
        for copy in self.loads(unit):
            copy.wait()
        self.over_rows(self.again_rows)

    def over_rows(self, work):
        def step(j, carry):
            work(pl.ds(pl.multiple_of(j * self.toks, self.toks), self.toks))
            return carry

        lax.fori_loop(0, 8, step, 0)

    def again_rows(self, rows):
        pre_act = jnp.dot(self.fbuf[1, rows], self.v1[:, :], preferred_element_type=F32).astype(BF16)
        self.ubuf[rows, :] = pre_act
        self.sbuf[rows, :] = gelu(pre_act.astype(F32)).astype(BF16)

    def again_back(self, rows):
        grad_post = lax.dot_general(self.fbuf[0, rows], self.v2[:, :], COL_CONTRACT, preferred_element_type=F32)
        pre_act = self.ubuf[rows, :].astype(F32)
        self.sbuf[rows, :] = (grad_post * gelu_slope(pre_act)).astype(BF16)

    def product(self, unit):
        if unit >= HELD:
            self.sent(unit - HELD)
        if self.kind(unit) == OUT:
            for copy in self.loads(unit):
                copy.wait()
        else:
            self.over_rows(self.again_back)
        sbuf, wp, edge = self.sbuf, self.wp.at[unit % HELD], self.edge
        block = edge // 2

        def step(b, carry):
            rows = pl.ds(pl.multiple_of(b * block, block), block)
            if self.kind(unit) == OUT:
                for part in range(2):
                    grads = self.fbuf[0, :, pl.ds(part * edge, edge)]
                    wp[part, rows] = lax.dot_general(sbuf[:, rows], grads, ROW_CONTRACT, preferred_element_type=F32)
            else:
                term = lax.dot_general(self.fbuf[1, :, rows], sbuf[:, :], ROW_CONTRACT, preferred_element_type=F32)
                wp[lax.div(b, 2), pl.ds(pl.multiple_of(lax.rem(b, 2) * block, block), block)] = term
            return carry

        lax.fori_loop(0, 2 if self.kind(unit) == OUT else 4, step, 0)
        for part in range(2):
            for way in range(2):
                self.rs(unit, part, 0, 0, way).start()


    def rs_axis(self, unit, part, phase):
        return self.axis(unit, 1 + (part + phase) % 2)

    @once
    def span(self, unit, part, phase, block, half=None):
        size = self.edge // RING
        base = 0
        if phase:
            base = self.at[self.rs_axis(unit, part, 0)] * size
            size //= RING
        row = base + self.ring(self.rs_axis(unit, part, phase), block) * size
        if half is not None:
            size //= 2
            row = row + half * size
        return pl.multiple_of(row, size), size

    @once
    def rs(self, unit, part, phase, step, way):
        if step == 0:
            row, size = self.span(unit, part, phase, 2, way)
            dst = self.near[phase]
        else:
            row, size = self.span(unit, part, phase, self.side(way))
            dst = self.far[phase]
        index = 10 + ((part * 2 + phase) * 2 + step) * 2 + way
        src = self.wp.at[unit % HELD, part, pl.ds(row, size)]
        return self.copy(unit, index, src, dst.at[unit, part, way], self.device(self.rs_axis(unit, part, phase), self.side(way)))

    def accumulate(self, unit, part, row, size, sources):
        chunk = min(16, size)

        def step(i, carry):
            at = pl.multiple_of(i * chunk, chunk)
            here = pl.ds(pl.multiple_of(row + at, chunk), chunk)
            total = self.wp[unit % HELD, part, here]
            for ref, way in sources:
                total = total + ref[unit, part, way, pl.ds(at, chunk)]
            self.wp[unit % HELD, part, here] = total
            return carry

        lax.fori_loop(0, size // chunk, step, 0)

    def reduce_near(self, unit, phase):
        for part in range(2):
            for way in range(2):
                self.rs(unit, part, phase, 0, way).wait_recv()
                row, size = self.span(unit, part, phase, self.side(way), way)
                self.accumulate(unit, part, row, size, [(self.near[phase], way)])
                self.rs(unit, part, phase, 1, way).start()

    def reduce_far(self, unit, phase):
        for part in range(2):
            for way in range(2):
                self.rs(unit, part, phase, 1, way).wait_recv()
            row, size = self.span(unit, part, phase, 0)
            self.accumulate(unit, part, row, size, [(self.far[phase], 0), (self.far[phase], 1)])
            for way in range(2):
                if phase == 0:
                    self.rs(unit, part, 1, 0, way).start()
                else:
                    self.ag(unit, part, 0, 0, way).start()
            if phase == 1:
                self.keep(unit, part).start()

    def reduce_2(self, unit):
        self.reduce_near(unit, 0)

    def reduce_3(self, unit):
        self.reduce_far(unit, 0)

    def reduce_4(self, unit):
        self.reduce_near(unit, 1)

    def reduce_5(self, unit):
        self.reduce_far(unit, 1)


    def result(self, unit, part, row, size, shift=None):
        layer, edge, piece = self.layer(unit), self.edge, self.piece
        if shift is None:
            first, count = self.core * RING, RING
        else:
            first, count = self.core * RING + self.ring(self.axis(unit, 0), shift), 1
        if self.kind(unit) == OUT:
            return self.r_out.at[layer, pl.ds(first, count), pl.ds(row, size), pl.ds(part * edge, edge)]
        cols = pl.ds(pl.multiple_of(first * piece, piece), count * piece)
        return self.r_in.at[layer, pl.ds(pl.multiple_of(part * edge + row, size), size), cols]

    def shard(self, unit, part):
        row, size = self.span(unit, part, 1, 0)
        return self.wp.at[unit % HELD, pl.ds(part, 1), pl.ds(row, size)] if self.kind(unit) == OUT else self.wp.at[unit % HELD, part, pl.ds(row, size)]

    @once
    def keep(self, unit, part):
        return pltpu.make_async_copy(
            self.shard(unit, part), self.result(unit, part, *self.span(unit, part, 1, 0), 0), self.own_sem.at[unit, part]
        )

    @once
    def ag(self, unit, part, phase, step, way):
        axis, block, half = self.rs_axis(unit, part, 0), 0, None
        if step:
            block, half = self.back(way), way
        if phase == 2:
            src = dst = self.result(unit, part, *self.span(unit, part, 0, block, half))
        elif (phase == 0) == ((unit, part) in CROSSED):
            axis = self.rs_axis(unit, part, 1)
            dst = self.result(unit, part, *self.span(unit, part, 1, block, half), 0 if phase == 0 else None)
            src = dst
        else:
            axis = self.axis(unit, 0)
            dst = self.result(unit, part, *self.span(unit, part, 1 - phase, 0, half), block)
            src = dst
        if phase == 0 and step == 0:
            src = self.shard(unit, part)
        index = 26 + ((part * 3 + phase) * 2 + step) * 2 + way
        return self.copy(unit, index, src, dst, self.device(axis, self.side(way)))

    @once
    def pair(self, unit, part, j):
        block, half = ((0, None), (3, None), (1, None), (2, 0), (2, 1))[j]
        ref = self.result(unit, part, *self.span(unit, part, 0, block, half))
        return self.copy(unit, 50 + part * 5 + j, ref, ref, self.partner())

    def gather_on(self, unit, phase):
        for part in range(2):
            for way in range(2):
                self.ag(unit, part, phase, 0, way).wait_recv()
                self.ag(unit, part, phase, 1, way).start()
                if phase == 2:
                    self.pair(unit, part, 1 + way).start()

    def gather_next(self, unit, phase):
        for part in range(2):
            for way in range(2):
                self.ag(unit, part, phase - 1, 1, way).wait_recv()
            if phase == 1:
                self.keep(unit, part).wait()
            for way in range(2):
                self.ag(unit, part, phase, 0, way).start()
            if phase == 2:
                self.pair(unit, part, 0).start()

    def gather_1(self, unit):
        self.gather_on(unit, 0)

    def gather_2(self, unit):
        self.gather_next(unit, 1)

    def gather_3(self, unit):
        self.gather_on(unit, 1)

    def gather_4(self, unit):
        self.gather_next(unit, 2)

    def gather_5(self, unit):
        self.gather_on(unit, 2)

    def gather_6(self, unit):
        for part in range(2):
            for way in range(2):
                self.ag(unit, part, 2, 1, way).wait_recv()
                self.pair(unit, part, 3 + way).start()

    def sent(self, unit):
        for part in range(2):
            for way in range(2):
                for step in range(2):
                    for phase in range(2):
                        self.rs(unit, part, phase, step, way).wait_send()
                self.ag(unit, part, 0, 0, way).wait_send()

    def finish(self, unit):
        if unit + HELD >= 2 * self.layers:
            self.sent(unit)
        for part in range(2):
            for j in range(5):
                self.pair(unit, part, j).wait()
            for way in range(2):
                self.ag(unit, part, 0, 1, way).wait_send()
                for step in range(2):
                    for phase in (1, 2):
                        self.ag(unit, part, phase, step, way).wait_send()
        for way in range(2):
            for later in range(2):
                self.full_out(unit, way, later).wait_send()
            self.full_on(unit, way).wait_send()
        for j in range(4):
            self.full_pair(unit, j).wait_send()

    def meet(self):
        barrier = pltpu.get_barrier_semaphore()
        others = [self.device(axis, shift) for axis in range(3) for shift in (1, 3)] + [self.partner()]
        for other in others:
            pl.semaphore_signal(barrier, inc=1, device_id=other, device_id_type=MESH)
        pl.semaphore_wait(barrier, len(others))

    def run(self):
        units = range(2 * self.layers)
        self.ahead(0, True)
        self.move(self.tokens, self.cur)
        self.meet()
        for code in ORDER:
            stage, unit = STAGES[code // 10], code % 10
            if unit < (self.layers if code < 20 else 2 * self.layers):
                getattr(self, stage)(unit)
        for unit in units:
            self.finish(unit)


def weight_grads(tokens, targets, w_in, w_out, inv_total):
    toks, dim = tokens.shape
    layers, _, hid = w_in.shape
    units, edge, piece, tile = 2 * layers, dim // 2, hid // 8, min(512, hid // 2)
    slots = min(4, hid // tile)
    assert edge == piece
    block, small = edge // RING, edge // RING**2

    def body(*refs):
        rest = refs[9:]
        near, far = (rest[4], rest[6]), (rest[5], rest[7])
        Reducer(refs[:4], refs[4:9], (*rest[:4], near, far, *rest[8:]), layers, toks, dim, hid, inv_total).run()

    anywhere = pl.BlockSpec(memory_space=pl.ANY)
    grad_in, grad_out, *_ = pl.pallas_call(
        body,
        in_specs=[anywhere] * 4,
        out_specs=[anywhere] * 5,
        out_shape=[
            jax.ShapeDtypeStruct((layers, dim, hid), F32),
            jax.ShapeDtypeStruct((layers, 8, piece, dim), F32),
            jax.ShapeDtypeStruct((units, 8, toks, dim), BF16),
            jax.ShapeDtypeStruct((layers, toks, dim), BF16),
            jax.ShapeDtypeStruct((layers, toks, dim), BF16),
        ],
        scratch_shapes=[
            pltpu.VMEM((2, 8 * toks, dim), BF16),
            pltpu.VMEM((8 * toks, piece), BF16),
            pltpu.VMEM((8 * toks, piece), BF16),
            pltpu.VMEM((min(HELD, units), 2, edge, edge), F32),
            pltpu.VMEM((units, 2, 2, block // 2, edge), F32),
            pltpu.VMEM((units, 2, 2, block, edge), F32),
            pltpu.VMEM((units, 2, 2, small // 2, edge), F32),
            pltpu.VMEM((units, 2, 2, small, edge), F32),
            pltpu.SemaphoreType.DMA((2, units, 60)),
            pltpu.SemaphoreType.DMA((2, 8)),
            pltpu.SemaphoreType.DMA((units + 1, 2)),
            pltpu.VMEM((toks, dim), BF16),
            pltpu.VMEM((toks, dim), F32),
            pltpu.VMEM((layers, toks, hid), BF16),
            pltpu.VMEM((slots, dim, tile), BF16),
            pltpu.VMEM((slots, tile, dim), BF16),
            pltpu.SemaphoreType.DMA((slots, 2)),
            pltpu.VMEM((dim, piece), BF16),
            pltpu.VMEM((piece, dim), BF16),
            pltpu.SemaphoreType.DMA((2,)),
        ],
        compiler_params=pltpu.CompilerParams(collective_id=1, has_side_effects=True, vmem_limit_bytes=63 << 20),
        cost_estimate=pl.CostEstimate(
            flops=16 * layers * toks * dim * hid, bytes_accessed=40 * layers * dim * hid, transcendentals=2 * layers * toks * hid
        ),
        name='weight_grads',
    )(tokens, targets, w_in, w_out)
    return grad_in, grad_out.reshape(layers, hid, dim)


def settle(arrays):
    blocks, ahead = 32, 4
    slots = 2 * ahead
    count = len(arrays)
    flat = [array.reshape(blocks, -1, array.shape[-1]) for array in arrays]

    def body(*refs):
        src, dst, held, sems = refs[:count], refs[count : 2 * count], refs[2 * count : 3 * count], refs[-1]

        def reads(i):
            slot = lax.rem(i, slots)
            return [pltpu.make_async_copy(src[k].at[i], held[k].at[slot], sems.at[0, k, slot]) for k in range(count)]

        def writes(i):
            slot = lax.rem(i, slots)
            return [pltpu.make_async_copy(held[k].at[slot], dst[k].at[i], sems.at[1, k, slot]) for k in range(count)]

        def step(i, carry):
            for read, write in zip(reads(i), writes(i)):
                read.wait()
                write.start()

            @pl.when((i >= ahead) & (i + ahead < blocks))
            def _():
                for write in writes(i - ahead):
                    write.wait()

            @pl.when(i + ahead < blocks)
            def _():
                for read in reads(i + ahead):
                    read.start()

            return carry

        def last(i, carry):
            for write in writes(i):
                write.wait()
            return carry

        for i in range(ahead):
            for read in reads(i):
                read.start()
        lax.fori_loop(0, blocks, step, 0)
        lax.fori_loop(blocks - slots, blocks, last, 0)

    anywhere = pl.BlockSpec(memory_space=pl.ANY)
    size = sum(array.size for array in arrays)
    out = pl.pallas_call(
        body,
        in_specs=[anywhere] * count,
        out_specs=[anywhere] * count,
        out_shape=[jax.ShapeDtypeStruct(x.shape, x.dtype) for x in flat],
        scratch_shapes=[pltpu.VMEM((slots, *x.shape[1:]), x.dtype) for x in flat] + [pltpu.SemaphoreType.DMA((2, count, slots))],
        compiler_params=pltpu.CompilerParams(vmem_limit_bytes=48 << 20),
        cost_estimate=pl.CostEstimate(flops=size, bytes_accessed=8 * size, transcendentals=0),
        name='settle',
    )(*flat)
    return [x.reshape(array.shape) for x, array in zip(out, arrays)]


def solution(mesh):
    def run(tokens, targets, w_in, w_out):
        inv_total = 1.0 / tokens.shape[0]

        def local_step(tok_local, tgt_local, w_first_all, w_second_all):
            return tuple(settle(weight_grads(tok_local, tgt_local, w_first_all, w_second_all, inv_total)))

        data_spec = P(DATA_AXES, None)
        mapped = jax.shard_map(local_step, mesh=mesh, in_specs=(data_spec, data_spec, P(), P()), out_specs=(P(), P()), check_vma=False)
        return mapped(tokens, targets, w_in, w_out)

    return run
```
